32 devices in a mesh: ax: 2 (over x), az: 16 (over z, y, core).
Axes of the slice: x: 2, y: 2, z: 4, core: 2. Of those that a mesh axis runs over, the one named last changes fastest.
Arguments:
- state: float32 [4, 8, 128, 2048], P(None, 'ax', 'az'), may hold values from -6 to 6
- rotor_offset: int32 [1], replicated, may hold values from 40 to 87
- rotor_fraction: float32 [1], replicated, may hold values from 0 to 1
Outputs:
- new_state: float32 [4, 8, 128, 2048], P(None, 'ax', 'az')
The draws below stay inside these ranges and needn't reach their ends.
All inputs are finite; a program needn't handle non-finite values.
Results may differ from the reference program's by a relative error of at most 0.00002.
Values sent between devices are 32-bit elements; how exact they have to be, the bound alone decides.
A program may use at most 64 MiB of HBM per device.

```python
import jax
import jax.numpy as jnp
from jax import lax

NV = 4
TH = 8
R = 2048
NP = 8
NTH = 128


def shard_levels(rng, extent, pieces, least, high):
    def one(axis_at, blocks):
        heights = jax.random.uniform(jax.random.fold_in(jax.random.fold_in(rng, 6), axis_at), (blocks,), jnp.float32, least / len(pieces), high / len(pieces))
        return jnp.repeat(jnp.exp(heights), extent[axis_at] // blocks).reshape((-1,) + (1,) * (len(extent) - axis_at - 1))

    gain = one(*pieces[0])
    for cut in pieces[1:]:
        gain = gain * one(*cut)
    return gain


def noise(rng, dims, scale, bound, split=(), kind=jnp.bfloat16):
    factor_of = shard_levels(rng, dims, split, -0.22, 0.18) if split else 1.0
    result = jax.random.normal(rng, dims, jnp.float32) * scale * factor_of
    return jnp.minimum(jnp.maximum(result, -bound), bound).astype(kind)


def setup_inputs(seed: int = 0) -> dict:
    splits = jax.random.split(jax.random.key(seed), 4)
    return {
        "state": noise(splits[0], (NV, NP, NTH, R), 1.0, 6.0, ((1, 2), (2, 16)), jnp.float32),
        "rotor_offset": jax.random.randint(splits[1], (1,), NTH // 4 + TH, 3 * NTH // 4 - TH).astype(jnp.int32),
        "rotor_fraction": jnp.clip(jax.random.uniform(splits[2], (1,), jnp.float32, 0.0, 1.0), 0.0, 1.0),
    }


step_size = 0.2
base_viscosity = 0.05
eddy_coeff = 0.05

def tendency(field, up_p, dn_p, up_t, dn_t, up_r, dn_r):
    grad_p = (up_p - dn_p) * 0.5
    grad_t = (up_t - dn_t) * 0.5
    grad_r = (up_r - dn_r) * 0.5
    second = up_p - 2.0 * field + dn_p + (up_t - 2.0 * field + dn_t) + (up_r - 2.0 * field + dn_r)
    strain = lax.optimization_barrier(jnp.sum(grad_p[:3] * grad_p[:3], axis=0)) + lax.optimization_barrier(jnp.sum(grad_t[:3] * grad_t[:3], axis=0)) + lax.optimization_barrier(jnp.sum(grad_r[:3] * grad_r[:3], axis=0))
    viscous = base_viscosity + eddy_coeff * jnp.sqrt(strain)
    advect = field[0] * grad_p + field[1] * grad_t + field[2] * grad_r
    return viscous * second - advect

def radial_sides(field, ghost_rot, ghost_sta):
    inner = field.shape[3] // 2
    zero = jnp.zeros(field.shape[:3] + (1,), field.dtype)
    up_r = jnp.concatenate([field[..., 1:inner], ghost_rot[..., None], field[..., inner + 1:], zero], axis=3)
    dn_r = jnp.concatenate([zero, field[..., :inner - 1], ghost_sta[..., None], field[..., inner:-1]], axis=3)
    return (up_r, dn_r)

def evaluate(field, offset, fraction):
    inner = field.shape[3] // 2
    stator_layer = field[..., inner]
    rotor_layer = field[..., inner - 1]
    ghost_rot = (1.0 - fraction) * jnp.roll(stator_layer, -offset, axis=2) + fraction * jnp.roll(stator_layer, -offset - 1, axis=2)
    ghost_sta = fraction * jnp.roll(rotor_layer, offset + 1, axis=2) + (1.0 - fraction) * jnp.roll(rotor_layer, offset, axis=2)
    zplane = jnp.zeros((field.shape[0], 1) + field.shape[2:], field.dtype)
    up_p = jnp.concatenate([field[:, 1:], zplane], axis=1)
    dn_p = jnp.concatenate([zplane, field[:, :-1]], axis=1)
    up_t = jnp.roll(field, -1, axis=2)
    dn_t = jnp.roll(field, 1, axis=2)
    up_r, dn_r = radial_sides(field, ghost_rot, ghost_sta)
    return tendency(field, up_p, dn_p, up_t, dn_t, up_r, dn_r)

def reference(state, rotor_offset, rotor_fraction):
    offset = rotor_offset[0]
    fraction = rotor_fraction[0]
    section = state + step_size * evaluate(state, offset, fraction)
    return 0.5 * (state + (section + step_size * evaluate(section, offset, fraction)))
```

```python
import functools

import jax
import jax.numpy as jnp
from jax import lax
from jax.experimental import pallas as pl
from jax.experimental.pallas import tpu as pltpu
from jax.sharding import PartitionSpec as P

step_size = 0.2
base_viscosity = 0.05
eddy_coeff = 0.05

LANE = 128
TILE = 256
CHUNK = 256


def kernel(n_ax, n_az, d_min, d_max, off_hbm, frac_hbm, state, out, q, s, t_send, t_recv, g_send, g_recv0, g_recv1,
           off_ref, frac_ref, load_sem, ax_send, ax_recv, az_send, az_recv, ag_send, ag_recv, ready):
    nv, planes, cells, radial = state.shape
    half = radial // 2
    wide = half + 2 * LANE
    per_half = half // CHUNK
    count = 2 * per_half
    edge = per_half - 1
    ax = lax.axis_index("ax")
    az = lax.axis_index("az")
    has_up = ax < n_ax - 1
    has_dn = ax > 0
    nxt = lax.rem(az + 1, n_az)
    prv = lax.rem(az + n_az - 1, n_az)
    reach = d_max - d_min + 1
    g_recv = (g_recv0, g_recv1)

    loads = [
        pltpu.make_async_copy(
            state.at[:, :, :, pl.ds(h * half, half)],
            q.at[:, pl.ds(1, planes), :, pl.ds(h * wide + LANE, half)],
            load_sem.at[h],
        )
        for h in range(2)
    ]
    scalars = [
        pltpu.make_async_copy(off_hbm, off_ref, load_sem.at[2]),
        pltpu.make_async_copy(frac_hbm, frac_ref, load_sem.at[3]),
    ]
    for load in loads + scalars:
        load.start()

    barrier = pltpu.get_barrier_semaphore()
    peers = [1, n_az - 1] + list(range(d_min, d_max + 1))

    def early(sector):
        return jnp.logical_and(lax.rem(sector, 2) == 0, sector < d_min)

    @pl.when(has_up)
    def _():
        pl.semaphore_signal(barrier, inc=1, device_id={"ax": ax + 1})

    @pl.when(has_dn)
    def _():
        pl.semaphore_signal(barrier, inc=1, device_id={"ax": ax - 1})

    for d in peers:
        peer = lax.rem(az + d, n_az)

        @pl.when(jnp.logical_not(early(peer)))
        def _(peer=peer):
            pl.semaphore_signal(barrier, inc=1, device_id={"az": peer})

    zero = jnp.zeros((cells, LANE), jnp.float32)
    for field in (q, s):
        for v in range(nv):
            for p in range(planes):
                field[v, p + 1, :, 0:LANE] = zero
                field[v, p + 1, :, 2 * wide - LANE :] = zero

        @pl.when(jnp.logical_not(has_dn))
        def _(field=field):
            for v in range(nv):
                field[v, 0, :, :] = jnp.zeros((cells, 2 * wide), jnp.float32)

        @pl.when(jnp.logical_not(has_up))
        def _(field=field):
            for v in range(nv):
                field[v, planes + 1, :, :] = jnp.zeros((cells, 2 * wide), jnp.float32)

    sub = lax.broadcasted_iota(jnp.int32, (cells, TILE), 0)
    sub1 = lax.broadcasted_iota(jnp.int32, (cells, LANE), 0)
    lane1 = lax.broadcasted_iota(jnp.int32, (cells, LANE), 1)

    for load in loads:
        load.wait()

    def axial(field, turn, index, up):
        h, c = index // per_half, index % per_half
        lanes = pl.ds(pl.multiple_of(h * wide + LANE + c * CHUNK, LANE), CHUNK)
        way = 0 if up else 1
        return pltpu.make_async_remote_copy(
            src_ref=field.at[:, planes if up else 1, :, lanes],
            dst_ref=field.at[:, 0 if up else planes + 1, :, lanes],
            send_sem=ax_send.at[turn, way, index],
            recv_sem=ax_recv.at[turn, way, index],
            device_id={"ax": ax + 1 if up else ax - 1},
        )

    def axial_start(field, turn, index):
        @pl.when(has_up)
        def _():
            axial(field, turn, index, True).start()

        @pl.when(has_dn)
        def _():
            axial(field, turn, index, False).start()

    def axial_wait(field, turn, index):
        @pl.when(has_dn)
        def _():
            axial(field, turn, index, True).wait_recv()

        @pl.when(has_up)
        def _():
            axial(field, turn, index, False).wait_recv()

    def axial_drain(field, turn, index):
        @pl.when(has_up)
        def _():
            axial(field, turn, index, True).wait_send()

        @pl.when(has_dn)
        def _():
            axial(field, turn, index, False).wait_send()

    def sector(turn, way, part):
        where = (slice(None), slice(None), slice(None), pl.ds(pl.multiple_of(part * CHUNK, LANE), CHUNK))
        return pltpu.make_async_remote_copy(
            src_ref=t_send.at[(turn, way) + where],
            dst_ref=t_recv.at[(turn, way) + where],
            send_sem=az_send.at[turn, way, part],
            recv_sem=az_recv.at[turn, way, part],
            device_id={"az": nxt if way == 0 else prv},
        )

    def spread(turn, d):
        return pltpu.make_async_remote_copy(
            src_ref=g_send.at[turn],
            dst_ref=g_recv[turn].at[d - d_min],
            send_sem=ag_send.at[turn, d - d_min],
            recv_sem=ag_recv.at[turn, d - d_min],
            device_id={"az": lax.rem(az + d, n_az)},
        )

    def pack_layers(field, turn):
        packed = zero
        for v in range(nv):
            for p in range(planes):
                index = v * planes + p
                stator = field[v, p + 1, :, wide + LANE : wide + 2 * LANE]
                rotor = field[v, p + 1, :, wide - 2 * LANE : wide - LANE]
                other = nv * planes + index
                if index:
                    stator = pltpu.roll(stator, index, 1)
                packed = jnp.where(lane1 == index, stator, packed)
                packed = jnp.where(lane1 == other, pltpu.roll(rotor, other + 1, 1), packed)
        g_send[turn] = packed

    def unpack_ghosts(field, turn):
        off = off_ref[0]
        f = frac_ref[0]

        def window(a, b, shift):
            turned = lax.rem(2 * cells - shift, cells)
            return jnp.where(sub1 < cells - shift, pltpu.roll(a, turned, 0), pltpu.roll(b, turned, 0))

        def between(start, lo, hi):
            k = jnp.clip(lax.div(start, cells), d_min, d_max - 1)
            r = lax.rem(start, cells)
            a = g_recv[turn][n_az - k - d_min]
            b = g_recv[turn][n_az - k - 1 - d_min]
            return lo * window(a, b, r) + hi * window(a, b, r + 1)

        rot = between(off, 1.0 - f, f)
        sta = between(n_az * cells - off - 1, f, 1.0 - f)
        for v in range(nv):
            for p in range(planes):
                index = v * planes + p
                other = nv * planes + index
                field[v, p + 1, :, wide - LANE : wide] = pltpu.roll(rot, LANE - index, 1) if index else rot
                field[v, p + 1, :, wide : wide + LANE] = pltpu.roll(sta, LANE - 1 - other, 1)

    def evaluate(field, turn, p, slot, base, tbase):
        values, grads, seconds = [], [], []
        strain = None
        for v in range(nv):
            ext = field[v, p + 1, :, pl.ds(base, TILE + 2 * LANE)]
            value = ext[:, LANE : LANE + TILE]
            up_r = pltpu.roll(ext, TILE + 2 * LANE - 1, 1)[:, LANE : LANE + TILE]
            dn_r = pltpu.roll(ext, 1, 1)[:, LANE : LANE + TILE]
            up_p = field[v, p + 2, :, pl.ds(base + LANE, TILE)]
            dn_p = field[v, p, :, pl.ds(base + LANE, TILE)]
            before = t_recv[turn, 0, slot, v, :, pl.ds(tbase, TILE)]
            after = t_recv[turn, 1, slot, v, :, pl.ds(tbase, TILE)]
            up_t = pltpu.roll(jnp.where(sub == 0, after, value), cells - 1, 0)
            dn_t = pltpu.roll(jnp.where(sub == cells - 1, before, value), 1, 0)
            grad = ((up_p - dn_p) * 0.5, (up_t - dn_t) * 0.5, (up_r - dn_r) * 0.5)
            second = (up_p + dn_p) + (up_t + dn_t) + (up_r + dn_r) - 6.0 * value
            if v < 3:
                square = grad[0] * grad[0] + grad[1] * grad[1] + grad[2] * grad[2]
                strain = square if strain is None else strain + square
            values.append(value)
            grads.append(grad)
            seconds.append(second)
        viscous = base_viscosity + eddy_coeff * jnp.sqrt(strain)
        steps = []
        for v in range(nv):
            advect = values[0] * grads[v][0] + values[1] * grads[v][1] + values[2] * grads[v][2]
            steps.append(step_size * (viscous * seconds[v] - advect))
        return values, steps

    def first(p, slot, base, tbase):
        values, steps = evaluate(q, 0, p, slot, base, tbase)
        for v in range(nv):
            section = values[v] + steps[v]
            s[v, p + 1, :, pl.ds(base + LANE, TILE)] = section
            t_send[1, 0, slot, v, :, pl.ds(tbase, TILE)] = section[cells - 1 :, :]
            t_send[1, 1, slot, v, :, pl.ds(tbase, TILE)] = section[0:1, :]

    def second(p, slot, base, tbase):
        values, steps = evaluate(s, 1, p, slot, base, tbase)
        for v in range(nv):
            before = q[v, p + 1, :, pl.ds(base + LANE, TILE)]
            out[v, p, :, pl.ds(tbase, TILE)] = 0.5 * (before + (values[v] + steps[v]))

    def evaluate_chunk(work, index):
        h, c = index // per_half, index % per_half
        base = pl.multiple_of(h * wide + c * CHUNK, LANE)
        tbase = pl.multiple_of(index * CHUNK, LANE)
        for p in range(planes):
            work(p, p, base, tbase)

    parts = range(count)
    pack_layers(q, 0)
    for slot in range(planes):
        p = slot
        for v in range(nv):
            for h in range(2):
                lanes = slice(h * wide + LANE, h * wide + LANE + half)
                t_send[0, 0, slot, v, :, h * half : (h + 1) * half] = q[v, p + 1, cells - 1 : cells, lanes]
                t_send[0, 1, slot, v, :, h * half : (h + 1) * half] = q[v, p + 1, 0:1, lanes]

    neighbours = has_up.astype(jnp.int32) + has_dn.astype(jnp.int32)
    pl.semaphore_wait(barrier, neighbours + jnp.where(early(az), 0, 2 + reach))

    order = [edge, edge + 1] + list(range(edge)) + list(range(edge + 2, count))
    for index in order:
        axial_start(q, 0, index)

    for d in peers:
        peer = lax.rem(az + d, n_az)

        @pl.when(early(peer))
        def _(peer=peer):
            pl.semaphore_signal(ready, inc=1, device_id={"az": peer})

    @pl.when(early(az))
    def _():
        pl.semaphore_wait(ready, 2 + reach)

    for d in range(d_min, d_max + 1):
        spread(0, d).start()
    for index in order:
        for way in range(2):
            sector(0, way, index).start()

    def run_first(low, high):
        @pl.loop(low, high)
        def _(index):
            for way in range(2):
                sector(0, way, index).wait_recv()
            axial_wait(q, 0, index)
            evaluate_chunk(first, index)
            axial_start(s, 1, index)
            for way in range(2):
                sector(1, way, index).start()

    def run_second(low, high):
        @pl.loop(low, high)
        def _(index):
            for way in range(2):
                sector(1, way, index).wait_recv()
            axial_wait(s, 1, index)
            evaluate_chunk(second, index)

    for d in range(d_min, d_max + 1):
        spread(0, d).wait_recv()
    for scalar in scalars:
        scalar.wait()
    unpack_ghosts(q, 0)
    run_first(edge, edge + 2)
    pack_layers(s, 1)
    for d in range(d_min, d_max + 1):
        spread(1, d).start()
    run_first(0, edge)
    run_first(edge + 2, count)

    run_second(0, edge)
    for d in range(d_min, d_max + 1):
        spread(1, d).wait_recv()
    unpack_ghosts(s, 1)
    run_second(edge, edge + 2)
    run_second(edge + 2, count)

    for turn, field in ((0, q), (1, s)):
        for d in range(d_min, d_max + 1):
            spread(turn, d).wait_send()
        for part in parts:
            for way in range(2):
                sector(turn, way, part).wait_send()
        for index in range(count):
            axial_drain(field, turn, index)


def shards(n_ax, n_az, state, rotor_offset, rotor_fraction):
    nv, planes, cells, radial = state.shape
    around = n_az * cells
    low, high = around // 4 + cells, 3 * around // 4 - cells - 1
    d_min, d_max = low // cells, high // cells + 1
    reach = d_max - d_min + 1
    wide = radial // 2 + 2 * LANE
    count = radial // CHUNK
    sem = pltpu.SemaphoreType.DMA
    return pl.pallas_call(
        functools.partial(kernel, n_ax, n_az, d_min, d_max),
        out_shape=jax.ShapeDtypeStruct(state.shape, state.dtype),
        in_specs=[
            pl.BlockSpec(memory_space=pltpu.HBM),
            pl.BlockSpec(memory_space=pltpu.HBM),
            pl.BlockSpec(memory_space=pltpu.HBM),
        ],
        out_specs=pl.BlockSpec(memory_space=pltpu.VMEM),
        scratch_shapes=[
            pltpu.VMEM((nv, planes + 2, cells, 2 * wide), jnp.float32),
            pltpu.VMEM((nv, planes + 2, cells, 2 * wide), jnp.float32),
            pltpu.VMEM((2, 2, planes, nv, 1, radial), jnp.float32),
            pltpu.VMEM((2, 2, planes, nv, 1, radial), jnp.float32),
            pltpu.VMEM((2, cells, LANE), jnp.float32),
            pltpu.VMEM((reach, cells, LANE), jnp.float32),
            pltpu.VMEM((reach, cells, LANE), jnp.float32),
            pltpu.SMEM((1,), jnp.int32),
            pltpu.SMEM((1,), jnp.float32),
            sem((4,)),
            sem((2, 2, count)),
            sem((2, 2, count)),
            sem((2, 2, count)),
            sem((2, 2, count)),
            sem((2, reach)),
            sem((2, reach)),
            pltpu.SemaphoreType.REGULAR,
        ],
        compiler_params=pltpu.CompilerParams(collective_id=0, has_side_effects=True, vmem_limit_bytes=55_000_000),
    )(rotor_offset, rotor_fraction, state)


def solution(mesh):
    return jax.shard_map(
        functools.partial(shards, mesh.shape["ax"], mesh.shape["az"]),
        mesh=mesh,
        in_specs=(P(None, "ax", "az", None), P(), P()),
        out_specs=P(None, "ax", "az", None),
        check_vma=False,
    )
```

```python
import functools

import jax
import jax.numpy as jnp
from jax import lax
from jax.experimental import pallas as pl
from jax.experimental.pallas import tpu as pltpu
from jax.sharding import PartitionSpec as P

step_size = 0.2
base_viscosity = 0.05
eddy_coeff = 0.05

LANE = 128
TILE = 256
CHUNK = 256


def kernel(n_ax, n_az, d_min, d_max, off_hbm, frac_hbm, state, out, q, s, t_send, t_recv, g_send, g_recv0, g_recv1,
           off_ref, frac_ref, load_sem, ax_send, ax_recv, az_send, az_recv, ag_send, ag_recv, ready):
    nv, planes, cells, radial = state.shape
    half = radial // 2
    wide = half + 2 * LANE
    per_half = half // CHUNK
    count = 2 * per_half
    edge = per_half - 1
    ax = lax.axis_index("ax")
    az = lax.axis_index("az")
    has_up = ax < n_ax - 1
    has_dn = ax > 0
    nxt = lax.rem(az + 1, n_az)
    prv = lax.rem(az + n_az - 1, n_az)
    g_recv = (g_recv0, g_recv1)

    def load(first, number, h, slot):
        return pltpu.make_async_copy(
            state.at[:, pl.ds(first, number), :, pl.ds(h * half, half)],
            q.at[:, pl.ds(first + 1, number), :, pl.ds(h * wide + LANE, half)],
            load_sem.at[slot, h],
        )

    outer_loads = [load(p, 1, h, i) for i, p in enumerate((0, planes - 1)) for h in range(2)]
    inner_loads = [load(1, planes - 2, h, 2) for h in range(2)]
    scalars = [
        pltpu.make_async_copy(off_hbm, off_ref, load_sem.at[3, 0]),
        pltpu.make_async_copy(frac_hbm, frac_ref, load_sem.at[3, 1]),
    ]
    for copy in outer_loads + inner_loads + scalars:
        copy.start()

    barrier = pltpu.get_barrier_semaphore()

    @pl.when(has_up)
    def _():
        pl.semaphore_signal(barrier, inc=1, device_id={"ax": ax + 1})

    @pl.when(has_dn)
    def _():
        pl.semaphore_signal(barrier, inc=1, device_id={"ax": ax - 1})

    layer_peers = list(range(d_min, d_max + 1))

    def sector_at(d):
        return lax.rem(az + d, n_az)

    def before(d):
        return sector_at(d) < az

    def number_before(ds):
        return sum(before(d).astype(jnp.int32) for d in ds)

    for d in [1, n_az - 1] + layer_peers:

        @pl.when(jnp.logical_not(before(d)))
        def _(d=d):
            pl.semaphore_signal(barrier, inc=1, device_id={"az": sector_at(d)})

    zero = jnp.zeros((cells, LANE), jnp.float32)

    sub = lax.broadcasted_iota(jnp.int32, (cells, TILE), 0)
    sub1 = lax.broadcasted_iota(jnp.int32, (cells, LANE), 0)
    lane1 = lax.broadcasted_iota(jnp.int32, (cells, LANE), 1)

    def axial(field, turn, index, up):
        h, c = index // per_half, index % per_half
        lanes = pl.ds(pl.multiple_of(h * wide + LANE + c * CHUNK, LANE), CHUNK)
        way = 0 if up else 1
        return pltpu.make_async_remote_copy(
            src_ref=field.at[:, planes if up else 1, :, lanes],
            dst_ref=field.at[:, 0 if up else planes + 1, :, lanes],
            send_sem=ax_send.at[turn, way, index],
            recv_sem=ax_recv.at[turn, way, index],
            device_id={"ax": ax + 1 if up else ax - 1},
        )

    def axial_start(field, turn, index):
        @pl.when(has_up)
        def _():
            axial(field, turn, index, True).start()

        @pl.when(has_dn)
        def _():
            axial(field, turn, index, False).start()

    def axial_wait(field, turn, index):
        @pl.when(has_dn)
        def _():
            axial(field, turn, index, True).wait_recv()

        @pl.when(has_up)
        def _():
            axial(field, turn, index, False).wait_recv()

    def axial_drain(field, turn, index):
        @pl.when(has_up)
        def _():
            axial(field, turn, index, True).wait_send()

        @pl.when(has_dn)
        def _():
            axial(field, turn, index, False).wait_send()

    def sector(turn, way, part):
        where = (slice(None), slice(None), slice(None), pl.ds(pl.multiple_of(part * CHUNK, LANE), CHUNK))
        return pltpu.make_async_remote_copy(
            src_ref=t_send.at[(turn, way) + where],
            dst_ref=t_recv.at[(turn, way) + where],
            send_sem=az_send.at[turn, way, part],
            recv_sem=az_recv.at[turn, way, part],
            device_id={"az": nxt if way == 0 else prv},
        )

    def spread(turn, d):
        return pltpu.make_async_remote_copy(
            src_ref=g_send.at[turn],
            dst_ref=g_recv[turn].at[d - d_min],
            send_sem=ag_send.at[turn, d - d_min],
            recv_sem=ag_recv.at[turn, d - d_min],
            device_id={"az": lax.rem(az + d, n_az)},
        )

    def pack_layers(field, turn):
        packed = zero
        for v in range(nv):
            for p in range(planes):
                index = v * planes + p
                stator = field[v, p + 1, :, wide + LANE : wide + 2 * LANE]
                rotor = field[v, p + 1, :, wide - 2 * LANE : wide - LANE]
                other = nv * planes + index
                if index:
                    stator = pltpu.roll(stator, index, 1)
                packed = jnp.where(lane1 == index, stator, packed)
                packed = jnp.where(lane1 == other, pltpu.roll(rotor, other + 1, 1), packed)
        g_send[turn] = packed

    def unpack_ghosts(field, turn):
        off = off_ref[0]
        f = frac_ref[0]

        def window(a, b, shift):
            turned = lax.rem(2 * cells - shift, cells)
            return jnp.where(sub1 < cells - shift, pltpu.roll(a, turned, 0), pltpu.roll(b, turned, 0))

        def between(start, lo, hi):
            k = jnp.clip(lax.div(start, cells), d_min, d_max - 1)
            r = lax.rem(start, cells)
            a = g_recv[turn][n_az - k - d_min]
            b = g_recv[turn][n_az - k - 1 - d_min]
            return lo * window(a, b, r) + hi * window(a, b, r + 1)

        rot = between(off, 1.0 - f, f)
        sta = between(n_az * cells - off - 1, f, 1.0 - f)
        for v in range(nv):
            for p in range(planes):
                index = v * planes + p
                other = nv * planes + index
                field[v, p + 1, :, wide - LANE : wide] = pltpu.roll(rot, LANE - index, 1) if index else rot
                field[v, p + 1, :, wide : wide + LANE] = pltpu.roll(sta, LANE - 1 - other, 1)

    def evaluate(field, turn, p, slot, base, tbase):
        values, grads, seconds = [], [], []
        strain = None
        for v in range(nv):
            ext = field[v, p + 1, :, pl.ds(base, TILE + 2 * LANE)]
            value = ext[:, LANE : LANE + TILE]
            up_r = pltpu.roll(ext, TILE + 2 * LANE - 1, 1)[:, LANE : LANE + TILE]
            dn_r = pltpu.roll(ext, 1, 1)[:, LANE : LANE + TILE]
            up_p = field[v, p + 2, :, pl.ds(base + LANE, TILE)]
            dn_p = field[v, p, :, pl.ds(base + LANE, TILE)]
            before = t_recv[turn, 0, slot, v, :, pl.ds(tbase, TILE)]
            after = t_recv[turn, 1, slot, v, :, pl.ds(tbase, TILE)]
            up_t = pltpu.roll(jnp.where(sub == 0, after, value), cells - 1, 0)
            dn_t = pltpu.roll(jnp.where(sub == cells - 1, before, value), 1, 0)
            grad = ((up_p - dn_p) * 0.5, (up_t - dn_t) * 0.5, (up_r - dn_r) * 0.5)
            second = (up_p + dn_p) + (up_t + dn_t) + (up_r + dn_r) - 6.0 * value
            if v < 3:
                square = grad[0] * grad[0] + grad[1] * grad[1] + grad[2] * grad[2]
                strain = square if strain is None else strain + square
            values.append(value)
            grads.append(grad)
            seconds.append(second)
        viscous = base_viscosity + eddy_coeff * jnp.sqrt(strain)
        steps = []
        for v in range(nv):
            advect = values[0] * grads[v][0] + values[1] * grads[v][1] + values[2] * grads[v][2]
            steps.append(step_size * (viscous * seconds[v] - advect))
        return values, steps

    def first(p, slot, base, tbase):
        values, steps = evaluate(q, 0, p, slot, base, tbase)
        for v in range(nv):
            section = values[v] + steps[v]
            s[v, p + 1, :, pl.ds(base + LANE, TILE)] = section
            t_send[1, 0, slot, v, :, pl.ds(tbase, TILE)] = section[cells - 1 :, :]
            t_send[1, 1, slot, v, :, pl.ds(tbase, TILE)] = section[0:1, :]

    def second(p, slot, base, tbase):
        values, steps = evaluate(s, 1, p, slot, base, tbase)
        for v in range(nv):
            before = q[v, p + 1, :, pl.ds(base + LANE, TILE)]
            out[v, p, :, pl.ds(tbase, TILE)] = 0.5 * (before + (values[v] + steps[v]))

    def evaluate_chunk(work, index, which):
        h, c = index // per_half, index % per_half
        base = pl.multiple_of(h * wide + c * CHUNK, LANE)
        tbase = pl.multiple_of(index * CHUNK, LANE)
        for p in which:
            work(p, p, base, tbase)

    neighbours = has_up.astype(jnp.int32) + has_dn.astype(jnp.int32)
    pl.semaphore_wait(barrier, neighbours + number_before([1, n_az - 1] + layer_peers))
    for d, slot in [(n_az - 1, 0), (1, 1)] + [(d, 2) for d in layer_peers]:

        @pl.when(before(d))
        def _(d=d, slot=slot):
            pl.semaphore_signal(ready.at[slot], inc=1, device_id={"az": sector_at(d)})

    for copy in outer_loads:
        copy.wait()
    parts = range(count)
    order = [edge, edge + 1] + list(range(edge)) + list(range(edge + 2, count))
    for index in order:
        axial_start(q, 0, index)

    for copy in inner_loads:
        copy.wait()
    for slot in range(planes):
        p = slot
        for v in range(nv):
            for h in range(2):
                lanes = slice(h * wide + LANE, h * wide + LANE + half)
                t_send[0, 0, slot, v, :, h * half : (h + 1) * half] = q[v, p + 1, cells - 1 : cells, lanes]
                t_send[0, 1, slot, v, :, h * half : (h + 1) * half] = q[v, p + 1, 0:1, lanes]

    def sector_start(way):
        for index in order:
            sector(0, way, index).start()

    @pl.when(before(n_az - 1))
    def _():
        sector_start(1)

    @pl.when(before(1))
    def _():
        sector_start(0)

    pack_layers(q, 0)
    for d in layer_peers:

        @pl.when(before(d))
        def _(d=d):
            spread(0, d).start()

    @pl.when(jnp.logical_not(before(1)))
    def _():
        pl.semaphore_wait(ready.at[0], 1)
        sector_start(0)

    for field in (q, s):
        for v in range(nv):
            for p in range(planes):
                field[v, p + 1, :, 0:LANE] = zero
                field[v, p + 1, :, 2 * wide - LANE :] = zero

        @pl.when(jnp.logical_not(has_dn))
        def _(field=field):
            for v in range(nv):
                field[v, 0, :, :] = jnp.zeros((cells, 2 * wide), jnp.float32)

        @pl.when(jnp.logical_not(has_up))
        def _(field=field):
            for v in range(nv):
                field[v, planes + 1, :, :] = jnp.zeros((cells, 2 * wide), jnp.float32)

    @pl.when(jnp.logical_not(before(n_az - 1)))
    def _():
        pl.semaphore_wait(ready.at[1], 1)
        sector_start(1)

    after = len(layer_peers) - number_before(layer_peers)

    @pl.when(after > 0)
    def _():
        pl.semaphore_wait(ready.at[2], after)

    for d in layer_peers:

        @pl.when(jnp.logical_not(before(d)))
        def _(d=d):
            spread(0, d).start()

    def run_first(low, high):
        @pl.loop(low, high)
        def _(index):
            for way in range(2):
                sector(0, way, index).wait_recv()
            axial_wait(q, 0, index)
            evaluate_chunk(first, index, range(planes))
            axial_start(s, 1, index)
            for way in range(2):
                sector(1, way, index).start()

    def run_second(low, high):
        @pl.loop(low, high)
        def _(index):
            for way in range(2):
                sector(1, way, index).wait_recv()
            evaluate_chunk(second, index, range(1, planes - 1))
            axial_wait(s, 1, index)
            evaluate_chunk(second, index, (0, planes - 1))

    for d in range(d_min, d_max + 1):
        spread(0, d).wait_recv()
    for scalar in scalars:
        scalar.wait()
    unpack_ghosts(q, 0)
    run_first(edge, edge + 2)
    pack_layers(s, 1)
    for d in range(d_min, d_max + 1):
        spread(1, d).start()
    run_first(0, edge)
    run_first(edge + 2, count)

    run_second(0, edge)
    run_second(edge + 2, count - 1)
    for d in range(d_min, d_max + 1):
        spread(1, d).wait_recv()
    unpack_ghosts(s, 1)
    run_second(edge, edge + 2)
    run_second(count - 1, count)

    for turn, field in ((0, q), (1, s)):
        for d in range(d_min, d_max + 1):
            spread(turn, d).wait_send()
        for part in parts:
            for way in range(2):
                sector(turn, way, part).wait_send()
        for index in range(count):
            axial_drain(field, turn, index)


def shards(n_ax, n_az, state, rotor_offset, rotor_fraction):
    nv, planes, cells, radial = state.shape
    around = n_az * cells
    low, high = around // 4 + cells, 3 * around // 4 - cells - 1
    d_min, d_max = low // cells, high // cells + 1
    reach = d_max - d_min + 1
    wide = radial // 2 + 2 * LANE
    count = radial // CHUNK
    sem = pltpu.SemaphoreType.DMA
    return pl.pallas_call(
        functools.partial(kernel, n_ax, n_az, d_min, d_max),
        out_shape=jax.ShapeDtypeStruct(state.shape, state.dtype),
        in_specs=[
            pl.BlockSpec(memory_space=pltpu.HBM),
            pl.BlockSpec(memory_space=pltpu.HBM),
            pl.BlockSpec(memory_space=pltpu.HBM),
        ],
        out_specs=pl.BlockSpec(memory_space=pltpu.VMEM),
        scratch_shapes=[
            pltpu.VMEM((nv, planes + 2, cells, 2 * wide), jnp.float32),
            pltpu.VMEM((nv, planes + 2, cells, 2 * wide), jnp.float32),
            pltpu.VMEM((2, 2, planes, nv, 1, radial), jnp.float32),
            pltpu.VMEM((2, 2, planes, nv, 1, radial), jnp.float32),
            pltpu.VMEM((2, cells, LANE), jnp.float32),
            pltpu.VMEM((reach, cells, LANE), jnp.float32),
            pltpu.VMEM((reach, cells, LANE), jnp.float32),
            pltpu.SMEM((1,), jnp.int32),
            pltpu.SMEM((1,), jnp.float32),
            sem((4, 2)),
            sem((2, 2, count)),
            sem((2, 2, count)),
            sem((2, 2, count)),
            sem((2, 2, count)),
            sem((2, reach)),
            sem((2, reach)),
            pltpu.SemaphoreType.REGULAR((3,)),
        ],
        compiler_params=pltpu.CompilerParams(collective_id=0, has_side_effects=True, vmem_limit_bytes=55_000_000),
    )(rotor_offset, rotor_fraction, state)


def solution(mesh):
    return jax.shard_map(
        functools.partial(shards, mesh.shape["ax"], mesh.shape["az"]),
        mesh=mesh,
        in_specs=(P(None, "ax", "az", None), P(), P()),
        out_specs=P(None, "ax", "az", None),
        check_vma=False,
    )
```

```python
import functools

import jax
import jax.numpy as jnp
from jax import lax
from jax.experimental import pallas as pl
from jax.experimental.pallas import tpu as pltpu
from jax.sharding import PartitionSpec as P

step_size = 0.2
base_viscosity = 0.05
eddy_coeff = 0.05

LANE = 128
TILE = 256
CHUNK = 256


def kernel(n_ax, n_az, d_min, d_max, off_hbm, frac_hbm, state, out, q, s, t_send, t_recv, g_send, g_recv0, g_recv1,
           off_ref, frac_ref, load_sem, ax_send, ax_recv, az_send, az_recv, ag_send, ag_recv, ready):
    nv, planes, cells, radial = state.shape
    half = radial // 2
    wide = half + 2 * LANE
    per_half = half // CHUNK
    count = 2 * per_half
    edge = per_half - 1
    g_recv = (g_recv0, g_recv1)
    ax = lax.axis_index("ax")
    az = lax.axis_index("az")
    has_up = ax < n_ax - 1
    has_dn = ax > 0
    nxt = lax.rem(az + 1, n_az)
    prv = lax.rem(az + n_az - 1, n_az)

    def load(first, number, h, slot):
        return pltpu.make_async_copy(
            state.at[:, pl.ds(first, number), :, pl.ds(h * half, half)],
            q.at[:, pl.ds(first + 1, number), :, pl.ds(h * wide + LANE, half)],
            load_sem.at[slot],
        )

    outer_loads = [load(p, 1, h, 0) for p in (0, planes - 1) for h in range(2)]
    inner_loads = [load(1, planes - 2, h, 1) for h in range(2)]
    scalars = [
        pltpu.make_async_copy(off_hbm, off_ref, load_sem.at[2]),
        pltpu.make_async_copy(frac_hbm, frac_ref, load_sem.at[3]),
    ]
    for copy in outer_loads + inner_loads + scalars:
        copy.start()

    def all_of(ref, semaphore):
        pltpu.make_async_copy(ref, ref, semaphore).wait()

    def loaded(number, slot):
        all_of(out.at[:, pl.ds(0, number)], load_sem.at[slot])

    barrier = pltpu.get_barrier_semaphore()

    layer_peers = list(range(d_min, d_max + 1))
    even = lax.rem(ax, 2) == 0
    first_even = jnp.logical_and(az == 0, even)
    first_odd = jnp.logical_and(az == 0, jnp.logical_not(even))

    def sector_at(d):
        return lax.rem(az + d, n_az)

    def before(d):
        return sector_at(d) < az

    def number_before(ds):
        return sum(before(d).astype(jnp.int32) for d in ds)

    def direct(d):
        return jnp.logical_and(jnp.logical_and(sector_at(d) == 0, even), d != n_az - 1)

    def signal_axial(semaphore, when):
        @pl.when(jnp.logical_and(when, has_up))
        def _():
            pl.semaphore_signal(semaphore, inc=1, device_id={"ax": ax + 1})

        @pl.when(jnp.logical_and(when, has_dn))
        def _():
            pl.semaphore_signal(semaphore, inc=1, device_id={"ax": ax - 1})

    signal_axial(barrier, jnp.logical_not(first_odd))
    for d in [1, n_az - 1] + layer_peers:

        @pl.when(jnp.logical_or(jnp.logical_not(before(d)), direct(d)))
        def _(d=d):
            pl.semaphore_signal(barrier, inc=1, device_id={"az": sector_at(d)})

    zero = jnp.zeros((cells, LANE), jnp.float32)

    sub = lax.broadcasted_iota(jnp.int32, (cells, TILE), 0)
    sub1 = lax.broadcasted_iota(jnp.int32, (cells, LANE), 0)
    lane1 = lax.broadcasted_iota(jnp.int32, (cells, LANE), 1)

    def axial(field, turn, index, up):
        h, c = index // per_half, index % per_half
        lanes = pl.ds(pl.multiple_of(h * wide + LANE + c * CHUNK, LANE), CHUNK)
        way = 0 if up else 1
        return pltpu.make_async_remote_copy(
            src_ref=field.at[:, planes if up else 1, :, lanes],
            dst_ref=field.at[:, 0 if up else planes + 1, :, lanes],
            send_sem=ax_send.at[way],
            recv_sem=ax_recv.at[turn, index],
            device_id={"ax": ax + 1 if up else ax - 1},
        )

    def axial_start(field, turn, index):
        @pl.when(has_up)
        def _():
            axial(field, turn, index, True).start()

        @pl.when(has_dn)
        def _():
            axial(field, turn, index, False).start()

    def axial_wait(turn, index):
        lanes = pl.ds(pl.multiple_of(index * CHUNK, LANE), CHUNK)

        @pl.when(jnp.logical_and(has_up, has_dn))
        def _():
            all_of(out.at[:, 0:2, :, lanes], ax_recv.at[turn, index])

        @pl.when(has_up != has_dn)
        def _():
            all_of(out.at[:, 0:1, :, lanes], ax_recv.at[turn, index])

    def sector(turn, way, part):
        where = (slice(None), slice(None), slice(None), pl.ds(pl.multiple_of(part * CHUNK, LANE), CHUNK))
        return pltpu.make_async_remote_copy(
            src_ref=t_send.at[(turn, way) + where],
            dst_ref=t_recv.at[(turn, way) + where],
            send_sem=az_send.at[0],
            recv_sem=az_recv.at[turn, part],
            device_id={"az": nxt if way == 0 else prv},
        )

    def sector_wait(turn, part):
        lanes = pl.ds(pl.multiple_of(part * CHUNK, LANE), CHUNK)
        all_of(t_recv.at[turn, :, :, :, :, lanes], az_recv.at[turn, part])

    def spread(turn, d):
        return pltpu.make_async_remote_copy(
            src_ref=g_send.at[turn],
            dst_ref=g_recv[turn].at[d - d_min],
            send_sem=ag_send.at[turn],
            recv_sem=ag_recv.at[turn],
            device_id={"az": lax.rem(az + d, n_az)},
        )

    def pack_layers(field, turn):
        packed = zero
        for v in range(nv):
            for p in range(planes):
                index = v * planes + p
                stator = field[v, p + 1, :, wide + LANE : wide + 2 * LANE]
                rotor = field[v, p + 1, :, wide - 2 * LANE : wide - LANE]
                other = nv * planes + index
                if index:
                    stator = pltpu.roll(stator, index, 1)
                packed = jnp.where(lane1 == index, stator, packed)
                packed = jnp.where(lane1 == other, pltpu.roll(rotor, other + 1, 1), packed)
        g_send[turn] = packed

    def unpack_ghosts(field, turn):
        off = off_ref[0]
        f = frac_ref[0]

        def window(a, b, shift):
            turned = lax.rem(2 * cells - shift, cells)
            return jnp.where(sub1 < cells - shift, pltpu.roll(a, turned, 0), pltpu.roll(b, turned, 0))

        def between(start, lo, hi):
            k = jnp.clip(lax.div(start, cells), d_min, d_max - 1)
            r = lax.rem(start, cells)
            a = g_recv[turn][n_az - k - d_min]
            b = g_recv[turn][n_az - k - 1 - d_min]
            return lo * window(a, b, r) + hi * window(a, b, r + 1)

        rot = between(off, 1.0 - f, f)
        sta = between(n_az * cells - off - 1, f, 1.0 - f)
        for v in range(nv):
            for p in range(planes):
                index = v * planes + p
                other = nv * planes + index
                field[v, p + 1, :, wide - LANE : wide] = pltpu.roll(rot, LANE - index, 1) if index else rot
                field[v, p + 1, :, wide : wide + LANE] = pltpu.roll(sta, LANE - 1 - other, 1)

    def evaluate(field, turn, p, slot, base, tbase):
        values, grads, seconds = [], [], []
        strain = None
        for v in range(nv):
            ext = field[v, p + 1, :, pl.ds(base, TILE + 2 * LANE)]
            value = ext[:, LANE : LANE + TILE]
            up_r = pltpu.roll(ext, TILE + 2 * LANE - 1, 1)[:, LANE : LANE + TILE]
            dn_r = pltpu.roll(ext, 1, 1)[:, LANE : LANE + TILE]
            up_p = field[v, p + 2, :, pl.ds(base + LANE, TILE)]
            dn_p = field[v, p, :, pl.ds(base + LANE, TILE)]
            before = t_recv[turn, 0, slot, v, :, pl.ds(tbase, TILE)]
            after = t_recv[turn, 1, slot, v, :, pl.ds(tbase, TILE)]
            up_t = pltpu.roll(jnp.where(sub == 0, after, value), cells - 1, 0)
            dn_t = pltpu.roll(jnp.where(sub == cells - 1, before, value), 1, 0)
            grad = ((up_p - dn_p) * 0.5, (up_t - dn_t) * 0.5, (up_r - dn_r) * 0.5)
            second = (up_p + dn_p) + (up_t + dn_t) + (up_r + dn_r) - 6.0 * value
            if v < 3:
                square = grad[0] * grad[0] + grad[1] * grad[1] + grad[2] * grad[2]
                strain = square if strain is None else strain + square
            values.append(value)
            grads.append(grad)
            seconds.append(second)
        viscous = base_viscosity + eddy_coeff * jnp.sqrt(strain)
        steps = []
        for v in range(nv):
            advect = values[0] * grads[v][0] + values[1] * grads[v][1] + values[2] * grads[v][2]
            steps.append(step_size * (viscous * seconds[v] - advect))
        return values, steps

    def first(p, slot, base, tbase):
        values, steps = evaluate(q, 0, p, slot, base, tbase)
        for v in range(nv):
            section = values[v] + steps[v]
            s[v, p + 1, :, pl.ds(base + LANE, TILE)] = section
            t_send[1, 0, slot, v, :, pl.ds(tbase, TILE)] = section[cells - 1 :, :]
            t_send[1, 1, slot, v, :, pl.ds(tbase, TILE)] = section[0:1, :]

    def second(p, slot, base, tbase):
        values, steps = evaluate(s, 1, p, slot, base, tbase)
        for v in range(nv):
            before = q[v, p + 1, :, pl.ds(base + LANE, TILE)]
            out[v, p, :, pl.ds(tbase, TILE)] = 0.5 * (before + (values[v] + steps[v]))

    def evaluate_chunk(work, index, which):
        h, c = index // per_half, index % per_half
        base = pl.multiple_of(h * wide + c * CHUNK, LANE)
        tbase = pl.multiple_of(index * CHUNK, LANE)
        for p in which:
            work(p, p, base, tbase)

    neighbours = has_up.astype(jnp.int32) + has_dn.astype(jnp.int32)

    @pl.when(jnp.logical_not(first_even))
    def _():
        pl.semaphore_wait(barrier, neighbours + number_before([1, n_az - 1] + layer_peers))

    signal_axial(ready.at[2], first_odd)
    for d, slot in [(n_az - 1, 0), (1, 1)] + [(d, 3 + n_az - d - d_min) for d in layer_peers]:

        @pl.when(jnp.logical_and(before(d), jnp.logical_not(direct(d))))
        def _(d=d, slot=slot):
            pl.semaphore_signal(ready.at[slot], inc=1, device_id={"az": sector_at(d)})

    @pl.when(first_even)
    def _():
        pl.semaphore_wait(ready.at[2], neighbours)

    loaded(2, 0)
    parts = range(count)
    order = [*range(edge), edge + 2, edge, edge + 1, *range(edge + 3, count)]
    for index in order:
        axial_start(q, 0, index)

    loaded(planes - 2, 1)
    pack_layers(q, 0)
    for d in layer_peers:

        @pl.when(before(d))
        def _(d=d):
            spread(0, d).start()

    for slot in range(planes):
        p = slot
        for v in range(nv):
            for h in range(2):
                lanes = slice(h * wide + LANE, h * wide + LANE + half)
                t_send[0, 0, slot, v, :, h * half : (h + 1) * half] = q[v, p + 1, cells - 1 : cells, lanes]
                t_send[0, 1, slot, v, :, h * half : (h + 1) * half] = q[v, p + 1, 0:1, lanes]

    def sector_start(way):
        for index in order:
            sector(0, way, index).start()

    @pl.when(before(n_az - 1))
    def _():
        sector_start(1)

    @pl.when(before(1))
    def _():
        sector_start(0)

    @pl.when(jnp.logical_not(before(1)))
    def _():
        pl.semaphore_wait(ready.at[0], 1)
        sector_start(0)

    for field in (q, s):
        for v in range(nv):
            for p in range(planes):
                field[v, p + 1, :, 0:LANE] = zero
                field[v, p + 1, :, 2 * wide - LANE :] = zero

        @pl.when(jnp.logical_not(has_dn))
        def _(field=field):
            for v in range(nv):
                field[v, 0, :, :] = jnp.zeros((cells, 2 * wide), jnp.float32)

        @pl.when(jnp.logical_not(has_up))
        def _(field=field):
            for v in range(nv):
                field[v, planes + 1, :, :] = jnp.zeros((cells, 2 * wide), jnp.float32)

    @pl.when(first_even)
    def _():
        pl.semaphore_wait(barrier, 1 + len(layer_peers))

    for d in layer_peers:

        @pl.when(jnp.logical_not(before(d)))
        def _(d=d):
            @pl.when(jnp.logical_not(first_even))
            def _():
                pl.semaphore_wait(ready.at[3 + d - d_min], 1)

            spread(0, d).start()

    @pl.when(first_odd)
    def _():
        pl.semaphore_wait(ready.at[1], 1)

    @pl.when(az == 0)
    def _():
        sector_start(1)

    def run_first(low, high):
        @pl.loop(low, high)
        def _(index):
            sector_wait(0, index)
            axial_wait(0, index)
            evaluate_chunk(first, index, range(planes))
            axial_start(s, 1, index)
            for way in range(2):
                sector(1, way, index).start()

    def run_second(low, high):
        @pl.loop(low, high)
        def _(index):
            sector_wait(1, index)
            evaluate_chunk(second, index, range(1, planes - 1))
            axial_wait(1, index)
            evaluate_chunk(second, index, (0, planes - 1))

    run_first(0, edge)
    run_first(edge + 2, edge + 3)
    split = jnp.where(az == n_az - 1, count, edge + 3)
    run_first(edge + 3, split)
    all_of(g_recv[0], ag_recv.at[0])
    for scalar in scalars:
        scalar.wait()
    unpack_ghosts(q, 0)
    run_first(edge, edge + 2)
    pack_layers(s, 1)
    for d in layer_peers:
        spread(1, d).start()
    run_first(split, count)

    run_second(0, edge)
    run_second(edge + 2, count)
    all_of(g_recv[1], ag_recv.at[1])
    unpack_ghosts(s, 1)
    run_second(edge, edge + 2)

    for turn in range(2):
        all_of(g_recv[turn], ag_send.at[turn])
    all_of(t_send, az_send.at[0])

    @pl.when(has_up)
    def _():
        all_of(out.at[:, 0:2], ax_send.at[0])

    @pl.when(has_dn)
    def _():
        all_of(out.at[:, 0:2], ax_send.at[1])


def shards(n_ax, n_az, state, rotor_offset, rotor_fraction):
    nv, planes, cells, radial = state.shape
    around = n_az * cells
    low, high = around // 4 + cells, 3 * around // 4 - cells - 1
    d_min, d_max = low // cells, high // cells + 1
    reach = d_max - d_min + 1
    wide = radial // 2 + 2 * LANE
    count = radial // CHUNK
    sem = pltpu.SemaphoreType.DMA
    return pl.pallas_call(
        functools.partial(kernel, n_ax, n_az, d_min, d_max),
        out_shape=jax.ShapeDtypeStruct(state.shape, state.dtype),
        in_specs=[
            pl.BlockSpec(memory_space=pltpu.HBM),
            pl.BlockSpec(memory_space=pltpu.HBM),
            pl.BlockSpec(memory_space=pltpu.HBM),
        ],
        out_specs=pl.BlockSpec(memory_space=pltpu.VMEM),
        scratch_shapes=[
            pltpu.VMEM((nv, planes + 2, cells, 2 * wide), jnp.float32),
            pltpu.VMEM((nv, planes + 2, cells, 2 * wide), jnp.float32),
            pltpu.VMEM((2, 2, planes, nv, 1, radial), jnp.float32),
            pltpu.VMEM((2, 2, planes, nv, 1, radial), jnp.float32),
            pltpu.VMEM((2, cells, LANE), jnp.float32),
            pltpu.VMEM((reach, cells, LANE), jnp.float32),
            pltpu.VMEM((reach, cells, LANE), jnp.float32),
            pltpu.SMEM((1,), jnp.int32),
            pltpu.SMEM((1,), jnp.float32),
            sem((4,)),
            sem((2,)),
            sem((2, count)),
            sem((1,)),
            sem((2, count)),
            sem((2,)),
            sem((2,)),
            pltpu.SemaphoreType.REGULAR((3 + reach,)),
        ],
        compiler_params=pltpu.CompilerParams(collective_id=0, has_side_effects=True, vmem_limit_bytes=55_000_000),
    )(rotor_offset, rotor_fraction, state)


def solution(mesh):
    return jax.shard_map(
        functools.partial(shards, mesh.shape["ax"], mesh.shape["az"]),
        mesh=mesh,
        in_specs=(P(None, "ax", "az", None), P(), P()),
        out_specs=P(None, "ax", "az", None),
        check_vma=False,
    )
```

```python
import functools

import jax
import jax.numpy as jnp
from jax import lax
from jax.experimental import pallas as pl
from jax.experimental.pallas import tpu as pltpu
from jax.sharding import PartitionSpec as P

step_size = 0.2
base_viscosity = 0.05
eddy_coeff = 0.05

LANE = 128
TILE = 256
CHUNK = 256
GROUPS = 3


def kernel(n_ax, n_az, d_min, d_max, off_ref, frac_ref, state, out, q, s, t_send, t_recv, g_send, g_recv0, g_recv1,
           load_sem, ax_send, az_send, ag_send, halo_recv, ax_recv, az_recv, ag_recv, ready):
    nv, planes, cells, radial = state.shape
    assert 2 * planes == cells
    half = radial // 2
    wide = half + 2 * LANE
    per_half = half // CHUNK
    count = 2 * per_half
    edge = per_half - 1
    g_recv = (g_recv0, g_recv1)
    ax = lax.axis_index("ax")
    az = lax.axis_index("az")
    has_up = ax < n_ax - 1
    has_dn = ax > 0
    nxt = lax.rem(az + 1, n_az)
    prv = lax.rem(az + n_az - 1, n_az)

    def load(first, number, h, slot):
        return pltpu.make_async_copy(
            state.at[:, pl.ds(first, number), :, pl.ds(h * half, half)],
            q.at[:, pl.ds(first + 1, number), :, pl.ds(h * wide + LANE, half)],
            load_sem.at[slot],
        )

    outer_loads = [load(p, 1, h, 0) for p in (0, planes - 1) for h in range(2)]
    inner_loads = [load(1, planes - 2, h, 1) for h in range(2)]
    for copy in outer_loads + inner_loads:
        copy.start()

    def all_of(ref, semaphore):
        pltpu.make_async_copy(ref, ref, semaphore).wait()

    def loaded(number, slot):
        all_of(out.at[:, pl.ds(0, number)], load_sem.at[slot])

    barrier = pltpu.get_barrier_semaphore()

    layer_peers = list(range(d_min, d_max + 1))
    even = lax.rem(ax, 2) == 0
    first_even = jnp.logical_and(az == 0, even)
    odd = jnp.logical_not(even)
    first_odd = jnp.logical_and(az == 0, odd)

    def group_of(d):
        return 3 + (d - d_min) * GROUPS // len(layer_peers)

    def sector_at(d):
        return lax.rem(az + d, n_az)

    def before(d):
        return sector_at(d) < az

    def number_before(ds):
        return sum(before(d).astype(jnp.int32) for d in ds)

    def direct(d):
        return jnp.logical_and(jnp.logical_and(sector_at(d) == 0, even), d != n_az - 1)

    def signal_axial(semaphore, when):
        @pl.when(jnp.logical_and(when, has_up))
        def _():
            pl.semaphore_signal(semaphore, inc=1, device_id={"ax": ax + 1})

        @pl.when(jnp.logical_and(when, has_dn))
        def _():
            pl.semaphore_signal(semaphore, inc=1, device_id={"ax": ax - 1})

    signal_axial(barrier, even)
    for d in [1, n_az - 1] + layer_peers:

        @pl.when(jnp.logical_or(jnp.logical_not(before(d)), direct(d)))
        def _(d=d):
            pl.semaphore_signal(barrier, inc=1, device_id={"az": sector_at(d)})

    zero = jnp.zeros((cells, LANE), jnp.float32)

    sub = lax.broadcasted_iota(jnp.int32, (cells, TILE), 0)
    sub1 = lax.broadcasted_iota(jnp.int32, (cells, LANE), 0)
    lane1 = lax.broadcasted_iota(jnp.int32, (cells, LANE), 1)

    def axial(field, turn, index, up):
        h, c = index // per_half, index % per_half
        lanes = pl.ds(pl.multiple_of(h * wide + LANE + c * CHUNK, LANE), CHUNK)
        way = 0 if up else 1
        return pltpu.make_async_remote_copy(
            src_ref=field.at[:, planes if up else 1, :, lanes],
            dst_ref=field.at[:, 0 if up else planes + 1, :, lanes],
            send_sem=ax_send.at[way],
            recv_sem=(ax_recv if turn else halo_recv).at[index],
            device_id={"ax": ax + 1 if up else ax - 1},
        )

    def axial_start(field, turn, index):
        @pl.when(has_up)
        def _():
            axial(field, turn, index, True).start()

        @pl.when(has_dn)
        def _():
            axial(field, turn, index, False).start()

    def planes_wait(semaphore, index, more):
        lanes = pl.ds(pl.multiple_of(index * CHUNK, LANE), CHUNK)

        @pl.when(jnp.logical_and(has_up, has_dn))
        def _():
            all_of(out.at[:, 0 : 2 + more, :, lanes], semaphore.at[index])

        @pl.when(has_up != has_dn)
        def _():
            all_of(out.at[:, 0 : 1 + more, :, lanes], semaphore.at[index])

        if more:

            @pl.when(jnp.logical_not(jnp.logical_or(has_up, has_dn)))
            def _():
                all_of(out.at[:, 0:more, :, lanes], semaphore.at[index])

    def sector(turn, way, part):
        where = (slice(None), slice(None), slice(None), pl.ds(pl.multiple_of(part * CHUNK, LANE), CHUNK))
        return pltpu.make_async_remote_copy(
            src_ref=t_send.at[(turn, way) + where],
            dst_ref=t_recv.at[(turn, way) + where],
            send_sem=az_send.at[0],
            recv_sem=(az_recv if turn else halo_recv).at[part],
            device_id={"az": nxt if way == 0 else prv},
        )

    def sector_wait(part):
        lanes = pl.ds(pl.multiple_of(part * CHUNK, LANE), CHUNK)
        all_of(t_recv.at[1, :, :, :, :, lanes], az_recv.at[part])

    def spread(turn, d):
        return pltpu.make_async_remote_copy(
            src_ref=g_send.at[turn],
            dst_ref=g_recv[turn].at[d - d_min],
            send_sem=ag_send.at[turn],
            recv_sem=ag_recv.at[turn],
            device_id={"az": lax.rem(az + d, n_az)},
        )

    def pack_layers(field, turn):
        packed = zero
        for v in range(nv):
            for p in range(planes):
                index = v * planes + p
                stator = field[v, p + 1, :, wide + LANE : wide + 2 * LANE]
                rotor = field[v, p + 1, :, wide - 2 * LANE : wide - LANE]
                other = nv * planes + index
                if index:
                    stator = pltpu.roll(stator, index, 1)
                packed = jnp.where(lane1 == index, stator, packed)
                packed = jnp.where(lane1 == other, pltpu.roll(rotor, other + 1, 1), packed)
        g_send[turn] = packed

    def unpack_ghosts(field, turn):
        off = off_ref[0]
        f = frac_ref[0]

        def window(a, b, shift):
            turned = lax.rem(2 * cells - shift, cells)
            return jnp.where(sub1 < cells - shift, pltpu.roll(a, turned, 0), pltpu.roll(b, turned, 0))

        def between(start, lo, hi):
            k = jnp.clip(lax.div(start, cells), d_min, d_max - 1)
            r = lax.rem(start, cells)
            a = g_recv[turn][n_az - k - d_min]
            b = g_recv[turn][n_az - k - 1 - d_min]
            return lo * window(a, b, r) + hi * window(a, b, r + 1)

        rot = between(off, 1.0 - f, f)
        sta = between(n_az * cells - off - 1, f, 1.0 - f)
        for v in range(nv):
            for p in range(planes):
                index = v * planes + p
                other = nv * planes + index
                field[v, p + 1, :, wide - LANE : wide] = pltpu.roll(rot, LANE - index, 1) if index else rot
                field[v, p + 1, :, wide : wide + LANE] = pltpu.roll(sta, LANE - 1 - other, 1)

    def evaluate(field, turn, p, slot, base, tbase):
        rates = [0.5 * step_size * field[v, p + 1, :, pl.ds(base + LANE, TILE)] for v in range(3)]
        moved, seconds = [], []
        strain = None
        for v in range(nv):
            ext = field[v, p + 1, :, pl.ds(base, TILE + 2 * LANE)]
            value = ext[:, LANE : LANE + TILE]
            up_r = pltpu.roll(ext, TILE + 2 * LANE - 1, 1)[:, LANE : LANE + TILE]
            dn_r = pltpu.roll(ext, 1, 1)[:, LANE : LANE + TILE]
            up_p = field[v, p + 2, :, pl.ds(base + LANE, TILE)]
            dn_p = field[v, p, :, pl.ds(base + LANE, TILE)]
            before = t_recv[turn, 0, slot, v, :, pl.ds(tbase, TILE)]
            after = t_recv[turn, 1, slot, v, :, pl.ds(tbase, TILE)]
            up_t = pltpu.roll(jnp.where(sub == 0, after, value), cells - 1, 0)
            dn_t = pltpu.roll(jnp.where(sub == cells - 1, before, value), 1, 0)
            across = (up_p - dn_p, up_t - dn_t, up_r - dn_r)
            seconds.append((up_p + dn_p) + (up_t + dn_t) + (up_r + dn_r) - 6.0 * value)
            moved.append(value - (rates[0] * across[0] + rates[1] * across[1] + rates[2] * across[2]))
            if v < 3:
                square = across[0] * across[0] + across[1] * across[1] + across[2] * across[2]
                strain = square if strain is None else strain + square
        viscous = step_size * base_viscosity + (0.5 * step_size * eddy_coeff) * jnp.sqrt(strain)
        return [moved[v] + viscous * seconds[v] for v in range(nv)]

    def first(p, slot, base, tbase):
        for v, section in enumerate(evaluate(q, 0, p, slot, base, tbase)):
            s[v, p + 1, :, pl.ds(base + LANE, TILE)] = section
            t_send[1, 0, slot, v, :, pl.ds(tbase, TILE)] = section[cells - 1 :, :]
            t_send[1, 1, slot, v, :, pl.ds(tbase, TILE)] = section[0:1, :]

    def second(p, slot, base, tbase):
        for v, stepped in enumerate(evaluate(s, 1, p, slot, base, tbase)):
            before = q[v, p + 1, :, pl.ds(base + LANE, TILE)]
            out[v, p, :, pl.ds(tbase, TILE)] = 0.5 * (before + stepped)

    def evaluate_chunk(work, index, which):
        h, c = index // per_half, index % per_half
        base = pl.multiple_of(h * wide + c * CHUNK, LANE)
        tbase = pl.multiple_of(index * CHUNK, LANE)
        for p in which:
            work(p, p, base, tbase)

    neighbours = has_up.astype(jnp.int32) + has_dn.astype(jnp.int32)

    @pl.when(jnp.logical_not(first_even))
    def _():
        pl.semaphore_wait(barrier, jnp.where(odd, neighbours, 0) + number_before([1, n_az - 1] + layer_peers))

    signal_axial(ready.at[2], odd)
    for d, slot in [(n_az - 1, 0), (1, 1)] + [(d, group_of(n_az - d)) for d in layer_peers]:

        @pl.when(jnp.logical_and(before(d), jnp.logical_not(direct(d))))
        def _(d=d, slot=slot):
            pl.semaphore_signal(ready.at[slot], inc=1, device_id={"az": sector_at(d)})

    loaded(2, 0)
    parts = range(count)
    last = jnp.logical_or(az == 0, az == n_az - 1)
    others = [*range(edge), *range(edge + 2, count)]
    order = [*others[: edge - 1], edge, edge + 1, *others[edge - 1 :]]
    order_last = [*others, edge, edge + 1]

    def planes_start():
        for index, index_last in zip(order, order_last):
            axial_start(q, 0, jnp.where(last, index_last, index))

    @pl.when(odd)
    def _():
        planes_start()

    loaded(planes - 2, 1)

    def pack_rows(way):
        row = slice(0, 1) if way else slice(cells - 1, cells)
        for p in range(planes):
            for v in range(nv):
                for h in range(2):
                    lanes = slice(h * wide + LANE, h * wide + LANE + half)
                    t_send[0, way, p, v, :, h * half : (h + 1) * half] = q[v, p + 1, row, lanes]

    def sector_start(way):
        to_last = az <= 1 if way else az >= n_az - 2
        for index, index_last in zip(order, order_last):
            sector(0, way, jnp.where(to_last, index_last, index)).start()

    @pl.when(az == n_az - 1)
    def _():
        pack_rows(0)
        sector_start(0)

    pack_layers(q, 0)
    for d in layer_peers:

        @pl.when(before(d))
        def _(d=d):
            spread(0, d).start()

    @pl.when(az < n_az - 1)
    def _():
        pack_rows(0)

    pack_rows(1)

    @pl.when(az > 0)
    def _():
        sector_start(1)

    @pl.when(even)
    def _():
        pl.semaphore_wait(ready.at[2], neighbours)
        planes_start()

    @pl.when(jnp.logical_not(before(1)))
    def _():
        pl.semaphore_wait(ready.at[0], 1)
        sector_start(0)

    for field in (q, s):
        for v in range(nv):
            for p in range(planes):
                field[v, p + 1, :, 0:LANE] = zero
                field[v, p + 1, :, 2 * wide - LANE :] = zero

        @pl.when(jnp.logical_not(has_dn))
        def _(field=field):
            for v in range(nv):
                field[v, 0, :, :] = jnp.zeros((cells, 2 * wide), jnp.float32)

        @pl.when(jnp.logical_not(has_up))
        def _(field=field):
            for v in range(nv):
                field[v, planes + 1, :, :] = jnp.zeros((cells, 2 * wide), jnp.float32)

    @pl.when(first_even)
    def _():
        pl.semaphore_wait(barrier, 1 + len(layer_peers))

    for group in range(3, 3 + GROUPS):
        members = [d for d in layer_peers if group_of(d) == group]
        after = len(members) - number_before(members)

        @pl.when(jnp.logical_and(after > 0, jnp.logical_not(first_even)))
        def _(group=group, after=after):
            pl.semaphore_wait(ready.at[group], after)

        for d in members:

            @pl.when(jnp.logical_not(before(d)))
            def _(d=d):
                spread(0, d).start()

    @pl.when(first_odd)
    def _():
        pl.semaphore_wait(ready.at[1], 1)

    @pl.when(az == 0)
    def _():
        sector_start(1)

    def other(place):
        return place + jnp.where(place < edge, 0, 2)

    def first_chunk(index, send):
        planes_wait(halo_recv, index, 1)
        evaluate_chunk(first, index, range(planes))

        @pl.when(send)
        def _():
            axial_start(s, 1, index)

        for way in range(2):
            sector(1, way, index).start()

    def second_chunk(index):
        sector_wait(index)
        evaluate_chunk(second, index, range(1, planes - 1))
        planes_wait(ax_recv, index, 0)
        evaluate_chunk(second, index, (0, planes - 1))

    def run_first(low, high):
        @pl.loop(low, high)
        def _(place):
            first_chunk(other(place), jnp.logical_or(az != 1, place < edge - 1))

    def run_second(low, high):
        @pl.loop(low, high)
        def _(place):
            second_chunk(other(place))

            @pl.when(jnp.logical_and(az == 1, place == edge - 2))
            def _():
                for index in others[edge - 1 :]:
                    axial_start(s, 1, index)

    split = jnp.where(last, len(others), edge - 1)
    run_first(0, split)
    all_of(g_recv[0], ag_recv.at[0])
    unpack_ghosts(q, 0)

    @pl.loop(edge, edge + 2)
    def _(index):
        first_chunk(index, True)

    pack_layers(s, 1)
    for d in layer_peers:
        spread(1, d).start()
    run_first(split, len(others))

    split = jnp.where(last, len(others), jnp.where(2 * az < n_az, edge + 1, edge - 1))
    run_second(0, split)
    all_of(g_recv[1], ag_recv.at[1])
    unpack_ghosts(s, 1)

    @pl.loop(edge, edge + 2)
    def _(index):
        second_chunk(index)

    run_second(split, len(others))

    for turn in range(2):
        all_of(g_recv[turn], ag_send.at[turn])
    all_of(t_send, az_send.at[0])

    @pl.when(has_up)
    def _():
        all_of(out.at[:, 0:2], ax_send.at[0])

    @pl.when(has_dn)
    def _():
        all_of(out.at[:, 0:2], ax_send.at[1])


def shards(n_ax, n_az, state, rotor_offset, rotor_fraction):
    nv, planes, cells, radial = state.shape
    around = n_az * cells
    low, high = around // 4 + cells, 3 * around // 4 - cells - 1
    d_min, d_max = low // cells, high // cells + 1
    reach = d_max - d_min + 1
    wide = radial // 2 + 2 * LANE
    count = radial // CHUNK
    sem = pltpu.SemaphoreType.DMA
    return pl.pallas_call(
        functools.partial(kernel, n_ax, n_az, d_min, d_max),
        out_shape=jax.ShapeDtypeStruct(state.shape, state.dtype),
        in_specs=[
            pl.BlockSpec(memory_space=pltpu.SMEM),
            pl.BlockSpec(memory_space=pltpu.SMEM),
            pl.BlockSpec(memory_space=pltpu.HBM),
        ],
        out_specs=pl.BlockSpec(memory_space=pltpu.VMEM),
        scratch_shapes=[
            pltpu.VMEM((nv, planes + 2, cells, 2 * wide), jnp.float32),
            pltpu.VMEM((nv, planes + 2, cells, 2 * wide), jnp.float32),
            pltpu.VMEM((2, 2, planes, nv, 1, radial), jnp.float32),
            pltpu.VMEM((2, 2, planes, nv, 1, radial), jnp.float32),
            pltpu.VMEM((2, cells, LANE), jnp.float32),
            pltpu.VMEM((reach, cells, LANE), jnp.float32),
            pltpu.VMEM((reach, cells, LANE), jnp.float32),
            sem((2,)),
            sem((2,)),
            sem((1,)),
            sem((2,)),
            sem((count,)),
            sem((count,)),
            sem((count,)),
            sem((2,)),
            pltpu.SemaphoreType.REGULAR((3 + GROUPS,)),
        ],
        compiler_params=pltpu.CompilerParams(collective_id=0, has_side_effects=True, vmem_limit_bytes=55_000_000),
    )(rotor_offset, rotor_fraction, state)


def solution(mesh):
    return jax.shard_map(
        functools.partial(shards, mesh.shape["ax"], mesh.shape["az"]),
        mesh=mesh,
        in_specs=(P(None, "ax", "az", None), P(), P()),
        out_specs=P(None, "ax", "az", None),
        check_vma=False,
    )
```

```python
import functools

import jax
import jax.numpy as jnp
from jax import lax
from jax.experimental import pallas as pl
from jax.experimental.pallas import tpu as pltpu
from jax.sharding import PartitionSpec as P

step_size = 0.2
base_viscosity = 0.05
eddy_coeff = 0.05

LANE = 128
TILE = 256
CHUNK = 256
GROUPS = 3


def kernel(n_ax, n_az, d_min, d_max, off_ref, frac_ref, state, out, q, s, pre_r, pre_t, pre_b, t_send, t_recv, g_send, g_recv0, g_recv1,
           load_sem, ax_send, az_send, ag_send, halo_recv, ax_recv, az_recv, ag_recv, ready):
    nv, planes, cells, radial = state.shape
    assert 2 * planes == cells
    half = radial // 2
    wide = half + 2 * LANE
    per_half = half // CHUNK
    count = 2 * per_half
    edge = per_half - 1
    g_recv = (g_recv0, g_recv1)
    ax = lax.axis_index("ax")
    az = lax.axis_index("az")
    has_up = ax < n_ax - 1
    has_dn = ax > 0
    nxt = lax.rem(az + 1, n_az)
    prv = lax.rem(az + n_az - 1, n_az)

    def load(first, number, h, slot):
        return pltpu.make_async_copy(
            state.at[:, pl.ds(first, number), :, pl.ds(h * half, half)],
            q.at[:, pl.ds(first + 1, number), :, pl.ds(h * wide + LANE, half)],
            load_sem.at[slot],
        )

    outer_loads = [load(p, 1, h, 0) for p in (0, planes - 1) for h in range(2)]
    inner_loads = [load(1, planes - 2, h, 1) for h in range(2)]
    for copy in outer_loads + inner_loads:
        copy.start()

    def all_of(ref, semaphore):
        pltpu.make_async_copy(ref, ref, semaphore).wait()

    def loaded(number, slot):
        all_of(out.at[:, pl.ds(0, number)], load_sem.at[slot])

    barrier = pltpu.get_barrier_semaphore()

    layer_peers = list(range(d_min, d_max + 1))
    even = lax.rem(ax, 2) == 0
    first_even = jnp.logical_and(az == 0, even)
    odd = jnp.logical_not(even)
    first_odd = jnp.logical_and(az == 0, odd)

    def group_of(d):
        return 3 + (d - d_min) * GROUPS // len(layer_peers)

    def sector_at(d):
        return lax.rem(az + d, n_az)

    def before(d):
        return sector_at(d) < az

    def number_before(ds):
        return sum(before(d).astype(jnp.int32) for d in ds)

    def direct(d):
        return jnp.logical_and(jnp.logical_and(sector_at(d) == 0, even), d != n_az - 1)

    def signal_axial(semaphore, when):
        @pl.when(jnp.logical_and(when, has_up))
        def _():
            pl.semaphore_signal(semaphore, inc=1, device_id={"ax": ax + 1})

        @pl.when(jnp.logical_and(when, has_dn))
        def _():
            pl.semaphore_signal(semaphore, inc=1, device_id={"ax": ax - 1})

    signal_axial(barrier, even)
    for d in [1, n_az - 1] + layer_peers:

        @pl.when(jnp.logical_or(jnp.logical_not(before(d)), direct(d)))
        def _(d=d):
            pl.semaphore_signal(barrier, inc=1, device_id={"az": sector_at(d)})

    zero = jnp.zeros((cells, LANE), jnp.float32)

    sub = lax.broadcasted_iota(jnp.int32, (cells, TILE), 0)
    sub1 = lax.broadcasted_iota(jnp.int32, (cells, LANE), 0)
    lane1 = lax.broadcasted_iota(jnp.int32, (cells, LANE), 1)

    def axial(field, turn, index, up):
        h, c = index // per_half, index % per_half
        lanes = pl.ds(pl.multiple_of(h * wide + LANE + c * CHUNK, LANE), CHUNK)
        way = 0 if up else 1
        return pltpu.make_async_remote_copy(
            src_ref=field.at[:, planes if up else 1, :, lanes],
            dst_ref=field.at[:, 0 if up else planes + 1, :, lanes],
            send_sem=ax_send.at[way],
            recv_sem=(ax_recv if turn else halo_recv).at[index],
            device_id={"ax": ax + 1 if up else ax - 1},
        )

    def axial_start(field, turn, index):
        @pl.when(has_up)
        def _():
            axial(field, turn, index, True).start()

        @pl.when(has_dn)
        def _():
            axial(field, turn, index, False).start()

    def planes_wait(semaphore, index, more):
        lanes = pl.ds(pl.multiple_of(index * CHUNK, LANE), CHUNK)

        @pl.when(jnp.logical_and(has_up, has_dn))
        def _():
            all_of(out.at[:, 0 : 2 + more, :, lanes], semaphore.at[index])

        @pl.when(has_up != has_dn)
        def _():
            all_of(out.at[:, 0 : 1 + more, :, lanes], semaphore.at[index])

        if more:

            @pl.when(jnp.logical_not(jnp.logical_or(has_up, has_dn)))
            def _():
                all_of(out.at[:, 0:more, :, lanes], semaphore.at[index])

    def sector(turn, way, part):
        where = (slice(None), slice(None), slice(None), pl.ds(pl.multiple_of(part * CHUNK, LANE), CHUNK))
        return pltpu.make_async_remote_copy(
            src_ref=t_send.at[(turn, way) + where],
            dst_ref=t_recv.at[(turn, way) + where],
            send_sem=az_send.at[0],
            recv_sem=(az_recv if turn else halo_recv).at[part],
            device_id={"az": nxt if way == 0 else prv},
        )

    def sector_wait(part):
        lanes = pl.ds(pl.multiple_of(part * CHUNK, LANE), CHUNK)
        all_of(t_recv.at[1, :, :, :, :, lanes], az_recv.at[part])

    def spread(turn, d):
        return pltpu.make_async_remote_copy(
            src_ref=g_send.at[turn],
            dst_ref=g_recv[turn].at[d - d_min],
            send_sem=ag_send.at[turn],
            recv_sem=ag_recv.at[turn],
            device_id={"az": lax.rem(az + d, n_az)},
        )

    def pack_layers(field, turn):
        packed = zero
        for v in range(nv):
            for p in range(planes):
                index = v * planes + p
                stator = field[v, p + 1, :, wide + LANE : wide + 2 * LANE]
                rotor = field[v, p + 1, :, wide - 2 * LANE : wide - LANE]
                other = nv * planes + index
                if index:
                    stator = pltpu.roll(stator, index, 1)
                packed = jnp.where(lane1 == index, stator, packed)
                packed = jnp.where(lane1 == other, pltpu.roll(rotor, other + 1, 1), packed)
        g_send[turn] = packed

    def unpack_ghosts(turn):
        off = off_ref[0]
        f = frac_ref[0]

        def window(a, b, shift):
            turned = lax.rem(2 * cells - shift, cells)
            return jnp.where(sub1 < cells - shift, pltpu.roll(a, turned, 0), pltpu.roll(b, turned, 0))

        def between(start, lo, hi):
            k = jnp.clip(lax.div(start, cells), d_min, d_max - 1)
            r = lax.rem(start, cells)
            a = g_recv[turn][n_az - k - d_min]
            b = g_recv[turn][n_az - k - 1 - d_min]
            return lo * window(a, b, r) + hi * window(a, b, r + 1)

        rot = between(off, 1.0 - f, f)
        sta = between(n_az * cells - off - 1, f, 1.0 - f)
        for v in range(nv):
            for p in range(planes):
                index = v * planes + p
                other = nv * planes + index
                ghost = jnp.where(lane1 == LANE - 1, pltpu.roll(rot, LANE - 1 - index, 1), 0.0)
                pre_r[v, p, :, half - LANE : half] += ghost
                pre_b[v, p, :, half - LANE : half] += ghost
                ghost = jnp.where(lane1 == 0, pltpu.roll(sta, LANE - other, 1), 0.0)
                pre_r[v, p, :, half : half + LANE] -= ghost
                pre_b[v, p, :, half : half + LANE] += ghost

    def prepare(field):
        @pl.loop(0, count)
        def _(index):
            h, c = index // per_half, index % per_half
            base = pl.multiple_of(h * wide + c * CHUNK, LANE)
            lanes = pl.ds(pl.multiple_of(index * CHUNK, LANE), TILE)
            for p in range(planes):
                for v in range(nv):
                    ext = field[v, p + 1, :, pl.ds(base, TILE + 2 * LANE)]
                    value = ext[:, LANE : LANE + TILE]
                    up_r = pltpu.roll(ext, TILE + 2 * LANE - 1, 1)[:, LANE : LANE + TILE]
                    dn_r = pltpu.roll(ext, 1, 1)[:, LANE : LANE + TILE]
                    up_t = jnp.where(sub == cells - 1, 0.0, pltpu.roll(value, cells - 1, 0))
                    dn_t = jnp.where(sub == 0, 0.0, pltpu.roll(value, 1, 0))
                    pre_r[v, p, :, lanes] = up_r - dn_r
                    pre_t[v, p, :, lanes] = up_t - dn_t
                    pre_b[v, p, :, lanes] = (up_t + dn_t) + (up_r + dn_r) - 6.0 * value

    def evaluate(field, turn, p, slot, base, tbase):
        rates = [0.5 * step_size * field[v, p + 1, :, pl.ds(base + LANE, TILE)] for v in range(3)]
        moved, seconds = [], []
        strain = None
        lanes = pl.ds(tbase, TILE)
        for v in range(nv):
            value = field[v, p + 1, :, pl.ds(base + LANE, TILE)]
            up_p = field[v, p + 2, :, pl.ds(base + LANE, TILE)]
            dn_p = field[v, p, :, pl.ds(base + LANE, TILE)]
            before = jnp.where(sub == 0, t_recv[turn, 0, slot, v, :, lanes], 0.0)
            after = jnp.where(sub == cells - 1, t_recv[turn, 1, slot, v, :, lanes], 0.0)
            across = (up_p - dn_p, pre_t[v, p, :, lanes] + (after - before), pre_r[v, p, :, lanes])
            seconds.append((up_p + dn_p) + (after + before) + pre_b[v, p, :, lanes])
            moved.append(value - (rates[0] * across[0] + rates[1] * across[1] + rates[2] * across[2]))
            if v < 3:
                square = across[0] * across[0] + across[1] * across[1] + across[2] * across[2]
                strain = square if strain is None else strain + square
        viscous = step_size * base_viscosity + (0.5 * step_size * eddy_coeff) * jnp.sqrt(strain)
        return [moved[v] + viscous * seconds[v] for v in range(nv)]

    def first(p, slot, base, tbase):
        for v, section in enumerate(evaluate(q, 0, p, slot, base, tbase)):
            s[v, p + 1, :, pl.ds(base + LANE, TILE)] = section
            t_send[1, 0, slot, v, :, pl.ds(tbase, TILE)] = section[cells - 1 :, :]
            t_send[1, 1, slot, v, :, pl.ds(tbase, TILE)] = section[0:1, :]

    def second(p, slot, base, tbase):
        for v, stepped in enumerate(evaluate(s, 1, p, slot, base, tbase)):
            before = q[v, p + 1, :, pl.ds(base + LANE, TILE)]
            out[v, p, :, pl.ds(tbase, TILE)] = 0.5 * (before + stepped)

    def evaluate_chunk(work, index, which):
        h, c = index // per_half, index % per_half
        base = pl.multiple_of(h * wide + c * CHUNK, LANE)
        tbase = pl.multiple_of(index * CHUNK, LANE)
        for p in which:
            work(p, p, base, tbase)

    neighbours = has_up.astype(jnp.int32) + has_dn.astype(jnp.int32)

    @pl.when(jnp.logical_not(first_even))
    def _():
        pl.semaphore_wait(barrier, jnp.where(odd, neighbours, 0) + number_before([1, n_az - 1] + layer_peers))

    signal_axial(ready.at[2], odd)
    for d, slot in [(n_az - 1, 0), (1, 1)] + [(d, group_of(n_az - d)) for d in layer_peers]:

        @pl.when(jnp.logical_and(before(d), jnp.logical_not(direct(d))))
        def _(d=d, slot=slot):
            pl.semaphore_signal(ready.at[slot], inc=1, device_id={"az": sector_at(d)})

    loaded(2, 0)
    parts = range(count)
    last = jnp.logical_or(az == 0, az == n_az - 1)
    others = [*range(edge), *range(edge + 2, count)]
    order = [*others[: edge - 1], edge, edge + 1, *others[edge - 1 :]]
    order_last = [*others, edge, edge + 1]

    def planes_start():
        for index, index_last in zip(order, order_last):
            axial_start(q, 0, jnp.where(last, index_last, index))

    @pl.when(odd)
    def _():
        planes_start()

    loaded(planes - 2, 1)

    def pack_rows(way):
        row = slice(0, 1) if way else slice(cells - 1, cells)
        for p in range(planes):
            for v in range(nv):
                for h in range(2):
                    lanes = slice(h * wide + LANE, h * wide + LANE + half)
                    t_send[0, way, p, v, :, h * half : (h + 1) * half] = q[v, p + 1, row, lanes]

    def sector_start(way):
        to_last = az <= 1 if way else az >= n_az - 2
        for index, index_last in zip(order, order_last):
            sector(0, way, jnp.where(to_last, index_last, index)).start()

    @pl.when(az == n_az - 1)
    def _():
        pack_rows(0)
        sector_start(0)

    pack_layers(q, 0)
    for d in layer_peers:

        @pl.when(before(d))
        def _(d=d):
            spread(0, d).start()

    @pl.when(az < n_az - 1)
    def _():
        pack_rows(0)

    pack_rows(1)

    @pl.when(az > 0)
    def _():
        sector_start(1)

    @pl.when(even)
    def _():
        pl.semaphore_wait(ready.at[2], neighbours)
        planes_start()

    @pl.when(jnp.logical_not(before(1)))
    def _():
        pl.semaphore_wait(ready.at[0], 1)
        sector_start(0)

    for field in (q, s):
        for v in range(nv):
            for p in range(planes):
                field[v, p + 1, :, 0:LANE] = zero
                field[v, p + 1, :, wide - LANE : wide + LANE] = jnp.zeros((cells, 2 * LANE), jnp.float32)
                field[v, p + 1, :, 2 * wide - LANE :] = zero

        @pl.when(jnp.logical_not(has_dn))
        def _(field=field):
            for v in range(nv):
                field[v, 0, :, :] = jnp.zeros((cells, 2 * wide), jnp.float32)

        @pl.when(jnp.logical_not(has_up))
        def _(field=field):
            for v in range(nv):
                field[v, planes + 1, :, :] = jnp.zeros((cells, 2 * wide), jnp.float32)

    prepare(q)

    @pl.when(first_even)
    def _():
        pl.semaphore_wait(barrier, 1 + len(layer_peers))

    for group in range(3, 3 + GROUPS):
        members = [d for d in layer_peers if group_of(d) == group]
        after = len(members) - number_before(members)

        @pl.when(jnp.logical_and(after > 0, jnp.logical_not(first_even)))
        def _(group=group, after=after):
            pl.semaphore_wait(ready.at[group], after)

        for d in members:

            @pl.when(jnp.logical_not(before(d)))
            def _(d=d):
                spread(0, d).start()

    @pl.when(first_odd)
    def _():
        pl.semaphore_wait(ready.at[1], 1)

    @pl.when(az == 0)
    def _():
        sector_start(1)

    def other(place):
        return place + jnp.where(place < edge, 0, 2)

    def first_chunk(index, send):
        planes_wait(halo_recv, index, 1)
        evaluate_chunk(first, index, range(planes))

        @pl.when(send)
        def _():
            axial_start(s, 1, index)

        for way in range(2):
            sector(1, way, index).start()

    def second_chunk(index):
        sector_wait(index)
        evaluate_chunk(second, index, range(1, planes - 1))
        planes_wait(ax_recv, index, 0)
        evaluate_chunk(second, index, (0, planes - 1))

    def run_first(low, high):
        @pl.loop(low, high)
        def _(place):
            first_chunk(other(place), jnp.logical_or(az != 1, place < edge - 1))

    def run_second(low, high):
        @pl.loop(low, high)
        def _(place):
            second_chunk(other(place))

            @pl.when(jnp.logical_and(az == 1, place == edge - 2))
            def _():
                for index in others[edge - 1 :]:
                    axial_start(s, 1, index)

    split = jnp.where(last, len(others), edge - 1)
    run_first(0, split)
    all_of(g_recv[0], ag_recv.at[0])
    unpack_ghosts(0)

    @pl.loop(edge, edge + 2)
    def _(index):
        first_chunk(index, True)

    pack_layers(s, 1)
    for d in layer_peers:
        spread(1, d).start()
    run_first(split, len(others))

    prepare(s)
    split = jnp.where(last, len(others), jnp.where(2 * az < n_az, edge + 1, edge - 1))
    run_second(0, split)
    all_of(g_recv[1], ag_recv.at[1])
    unpack_ghosts(1)

    @pl.loop(edge, edge + 2)
    def _(index):
        second_chunk(index)

    run_second(split, len(others))

    for turn in range(2):
        all_of(g_recv[turn], ag_send.at[turn])
    all_of(t_send, az_send.at[0])

    @pl.when(has_up)
    def _():
        all_of(out.at[:, 0:2], ax_send.at[0])

    @pl.when(has_dn)
    def _():
        all_of(out.at[:, 0:2], ax_send.at[1])


def shards(n_ax, n_az, state, rotor_offset, rotor_fraction):
    nv, planes, cells, radial = state.shape
    around = n_az * cells
    low, high = around // 4 + cells, 3 * around // 4 - cells - 1
    d_min, d_max = low // cells, high // cells + 1
    reach = d_max - d_min + 1
    wide = radial // 2 + 2 * LANE
    count = radial // CHUNK
    sem = pltpu.SemaphoreType.DMA
    return pl.pallas_call(
        functools.partial(kernel, n_ax, n_az, d_min, d_max),
        out_shape=jax.ShapeDtypeStruct(state.shape, state.dtype),
        in_specs=[
            pl.BlockSpec(memory_space=pltpu.SMEM),
            pl.BlockSpec(memory_space=pltpu.SMEM),
            pl.BlockSpec(memory_space=pltpu.HBM),
        ],
        out_specs=pl.BlockSpec(memory_space=pltpu.VMEM),
        scratch_shapes=[
            pltpu.VMEM((nv, planes + 2, cells, 2 * wide), jnp.float32),
            pltpu.VMEM((nv, planes + 2, cells, 2 * wide), jnp.float32),
            pltpu.VMEM(state.shape, jnp.float32),
            pltpu.VMEM(state.shape, jnp.float32),
            pltpu.VMEM(state.shape, jnp.float32),
            pltpu.VMEM((2, 2, planes, nv, 1, radial), jnp.float32),
            pltpu.VMEM((2, 2, planes, nv, 1, radial), jnp.float32),
            pltpu.VMEM((2, cells, LANE), jnp.float32),
            pltpu.VMEM((reach, cells, LANE), jnp.float32),
            pltpu.VMEM((reach, cells, LANE), jnp.float32),
            sem((2,)),
            sem((2,)),
            sem((1,)),
            sem((2,)),
            sem((count,)),
            sem((count,)),
            sem((count,)),
            sem((2,)),
            pltpu.SemaphoreType.REGULAR((3 + GROUPS,)),
        ],
        compiler_params=pltpu.CompilerParams(collective_id=0, has_side_effects=True, vmem_limit_bytes=55_000_000),
    )(rotor_offset, rotor_fraction, state)


def solution(mesh):
    return jax.shard_map(
        functools.partial(shards, mesh.shape["ax"], mesh.shape["az"]),
        mesh=mesh,
        in_specs=(P(None, "ax", "az", None), P(), P()),
        out_specs=P(None, "ax", "az", None),
        check_vma=False,
    )
```

```python
import functools

import jax
import jax.numpy as jnp
from jax import lax
from jax.experimental import pallas as pl
from jax.experimental.pallas import tpu as pltpu
from jax.sharding import PartitionSpec as P

step_size = 0.2
base_viscosity = 0.05
eddy_coeff = 0.05

LANE = 128
TILE = 256
CHUNK = 256
GROUPS = 3


def kernel(n_ax, n_az, d_min, d_max, off_ref, frac_ref, state, out, q, s, pre_r, pre_t, pre_b, t_send, t_recv, g_send, g_recv0, g_recv1,
           load_sem, halo_send, ag_send, halo_recv, ax_recv, az_recv, ag_recv, ready):
    nv, planes, cells, radial = state.shape
    assert 2 * planes == cells and planes >= 4
    half = radial // 2
    wide = half + 2 * LANE
    per_half = half // CHUNK
    count = 2 * per_half
    edge = per_half - 1
    g_recv = (g_recv0, g_recv1)
    ax = lax.axis_index("ax")
    az = lax.axis_index("az")
    has_up = ax < n_ax - 1
    has_dn = ax > 0
    nxt = lax.rem(az + 1, n_az)
    prv = lax.rem(az + n_az - 1, n_az)

    def load(first, number, h, slot):
        return pltpu.make_async_copy(
            state.at[:, pl.ds(first, number), :, pl.ds(h * half, half)],
            q.at[:, pl.ds(first + 1, number), :, pl.ds(h * wide + LANE, half)],
            load_sem.at[slot],
        )

    even = lax.rem(ax, 2) == 0
    odd = jnp.logical_not(even)
    bottom_loads = [load(0, 1, h, 0) for h in range(2)]
    top_loads = [load(planes - 1, 1, h, 1) for h in range(2)]

    @pl.when(even)
    def _():
        for copy in top_loads + bottom_loads:
            copy.start()

    @pl.when(odd)
    def _():
        for copy in bottom_loads + top_loads:
            copy.start()

    for h in range(2):
        load(1, planes - 2, h, 2).start()

    def all_of(ref, semaphore):
        pltpu.make_async_copy(ref, ref, semaphore).wait()

    def loaded(number, slot):
        all_of(out.at[:, pl.ds(0, number)], load_sem.at[slot])

    barrier = pltpu.get_barrier_semaphore()

    layer_peers = list(range(d_min, d_max + 1))
    first_even = jnp.logical_and(az == 0, even)
    first_odd = jnp.logical_and(az == 0, odd)

    def group_of(d):
        return 2 + (d - d_min) * GROUPS // len(layer_peers)

    def sector_at(d):
        return lax.rem(az + d, n_az)

    def before(d):
        return sector_at(d) < az

    def number_before(ds):
        return sum(before(d).astype(jnp.int32) for d in ds)

    def direct(d):
        return jnp.logical_and(jnp.logical_and(sector_at(d) == 0, even), d != n_az - 1)

    def signal_axial(semaphore, when):
        @pl.when(jnp.logical_and(when, has_up))
        def _():
            pl.semaphore_signal(semaphore, inc=1, device_id={"ax": ax + 1})

        @pl.when(jnp.logical_and(when, has_dn))
        def _():
            pl.semaphore_signal(semaphore, inc=1, device_id={"ax": ax - 1})

    signal_axial(barrier, even)
    for d in [1, n_az - 1] + layer_peers:

        @pl.when(jnp.logical_or(jnp.logical_not(before(d)), direct(d)))
        def _(d=d):
            pl.semaphore_signal(barrier, inc=1, device_id={"az": sector_at(d)})

    zero = jnp.zeros((cells, LANE), jnp.float32)

    sub = lax.broadcasted_iota(jnp.int32, (cells, TILE), 0)
    sub1 = lax.broadcasted_iota(jnp.int32, (cells, LANE), 0)
    lane1 = lax.broadcasted_iota(jnp.int32, (cells, LANE), 1)

    def axial(field, turn, index, up):
        h, c = index // per_half, index % per_half
        lanes = pl.ds(pl.multiple_of(h * wide + LANE + c * CHUNK, LANE), CHUNK)
        way = 0 if up else 1
        return pltpu.make_async_remote_copy(
            src_ref=field.at[:, planes if up else 1, :, lanes],
            dst_ref=field.at[:, 0 if up else planes + 1, :, lanes],
            send_sem=halo_send.at[0],
            recv_sem=(ax_recv if turn else halo_recv).at[index],
            device_id={"ax": ax + 1 if up else ax - 1},
        )

    def axial_start(field, turn, index):
        @pl.when(has_up)
        def _():
            axial(field, turn, index, True).start()

        @pl.when(has_dn)
        def _():
            axial(field, turn, index, False).start()

    def planes_wait(semaphore, index, more):
        lanes = pl.ds(pl.multiple_of(index * CHUNK, LANE), CHUNK)

        @pl.when(jnp.logical_and(has_up, has_dn))
        def _():
            all_of(out.at[:, 0 : 2 + more, :, lanes], semaphore.at[index])

        @pl.when(has_up != has_dn)
        def _():
            all_of(out.at[:, 0 : 1 + more, :, lanes], semaphore.at[index])

        if more:

            @pl.when(jnp.logical_not(jnp.logical_or(has_up, has_dn)))
            def _():
                all_of(out.at[:, 0:more, :, lanes], semaphore.at[index])

    def sector(turn, way, part):
        where = (slice(None), slice(None), slice(None), pl.ds(pl.multiple_of(part * CHUNK, LANE), CHUNK))
        return pltpu.make_async_remote_copy(
            src_ref=t_send.at[(turn, way) + where],
            dst_ref=t_recv.at[(turn, way) + where],
            send_sem=halo_send.at[0],
            recv_sem=(az_recv if turn else halo_recv).at[part],
            device_id={"az": nxt if way == 0 else prv},
        )

    def sector_wait(part):
        lanes = pl.ds(pl.multiple_of(part * CHUNK, LANE), CHUNK)
        all_of(t_recv.at[1, :, :, :, :, lanes], az_recv.at[part])

    def spread(turn, d):
        return pltpu.make_async_remote_copy(
            src_ref=g_send.at[turn],
            dst_ref=g_recv[turn].at[d - d_min],
            send_sem=ag_send.at[turn],
            recv_sem=ag_recv.at[turn],
            device_id={"az": lax.rem(az + d, n_az)},
        )

    def pack_layers(field, turn):
        packed = zero
        for v in range(nv):
            for p in range(planes):
                index = v * planes + p
                stator = field[v, p + 1, :, wide + LANE : wide + 2 * LANE]
                rotor = field[v, p + 1, :, wide - 2 * LANE : wide - LANE]
                other = nv * planes + index
                if index:
                    stator = pltpu.roll(stator, index, 1)
                packed = jnp.where(lane1 == index, stator, packed)
                packed = jnp.where(lane1 == other, pltpu.roll(rotor, other + 1, 1), packed)
        g_send[turn] = packed

    def unpack_ghosts(turn):
        off = off_ref[0]
        f = frac_ref[0]

        def window(a, b, shift):
            turned = lax.rem(2 * cells - shift, cells)
            return jnp.where(sub1 < cells - shift, pltpu.roll(a, turned, 0), pltpu.roll(b, turned, 0))

        def between(start, lo, hi):
            k = jnp.clip(lax.div(start, cells), d_min, d_max - 1)
            r = lax.rem(start, cells)
            a = g_recv[turn][n_az - k - d_min]
            b = g_recv[turn][n_az - k - 1 - d_min]
            return lo * window(a, b, r) + hi * window(a, b, r + 1)

        rot = between(off, 1.0 - f, f)
        sta = between(n_az * cells - off - 1, f, 1.0 - f)
        for v in range(nv):
            for p in range(planes):
                index = v * planes + p
                other = nv * planes + index
                ghost = jnp.where(lane1 == LANE - 1, pltpu.roll(rot, LANE - 1 - index, 1), 0.0)
                pre_r[v, p, :, half - LANE : half] += ghost
                pre_b[v, p, :, half - LANE : half] += ghost
                ghost = jnp.where(lane1 == 0, pltpu.roll(sta, LANE - other, 1), 0.0)
                pre_r[v, p, :, half : half + LANE] -= ghost
                pre_b[v, p, :, half : half + LANE] += ghost

    def prepare(field, low=0, high=count):
        @pl.loop(low, high)
        def _(index):
            h, c = index // per_half, index % per_half
            base = pl.multiple_of(h * wide + c * CHUNK, LANE)
            lanes = pl.ds(pl.multiple_of(index * CHUNK, LANE), TILE)
            for p in range(planes):
                for v in range(nv):
                    ext = field[v, p + 1, :, pl.ds(base, TILE + 2 * LANE)]
                    value = ext[:, LANE : LANE + TILE]
                    up_r = pltpu.roll(ext, TILE + 2 * LANE - 1, 1)[:, LANE : LANE + TILE]
                    dn_r = pltpu.roll(ext, 1, 1)[:, LANE : LANE + TILE]
                    up_t = jnp.where(sub == cells - 1, 0.0, pltpu.roll(value, cells - 1, 0))
                    dn_t = jnp.where(sub == 0, 0.0, pltpu.roll(value, 1, 0))
                    pre_r[v, p, :, lanes] = up_r - dn_r
                    pre_t[v, p, :, lanes] = up_t - dn_t
                    pre_b[v, p, :, lanes] = (up_t + dn_t) + (up_r + dn_r) - 6.0 * value

    def evaluate(field, turn, p, slot, base, tbase):
        rates = [0.5 * step_size * field[v, p + 1, :, pl.ds(base + LANE, TILE)] for v in range(3)]
        moved, seconds = [], []
        strain = None
        lanes = pl.ds(tbase, TILE)
        for v in range(nv):
            value = field[v, p + 1, :, pl.ds(base + LANE, TILE)]
            up_p = field[v, p + 2, :, pl.ds(base + LANE, TILE)]
            dn_p = field[v, p, :, pl.ds(base + LANE, TILE)]
            before = jnp.where(sub == 0, t_recv[turn, 0, slot, v, :, lanes], 0.0)
            after = jnp.where(sub == cells - 1, t_recv[turn, 1, slot, v, :, lanes], 0.0)
            across = (up_p - dn_p, pre_t[v, p, :, lanes] + (after - before), pre_r[v, p, :, lanes])
            seconds.append((up_p + dn_p) + (after + before) + pre_b[v, p, :, lanes])
            moved.append(value - (rates[0] * across[0] + rates[1] * across[1] + rates[2] * across[2]))
            if v < 3:
                square = across[0] * across[0] + across[1] * across[1] + across[2] * across[2]
                strain = square if strain is None else strain + square
        viscous = step_size * base_viscosity + (0.5 * step_size * eddy_coeff) * jnp.sqrt(strain)
        return [moved[v] + viscous * seconds[v] for v in range(nv)]

    def first(p, slot, base, tbase):
        for v, section in enumerate(evaluate(q, 0, p, slot, base, tbase)):
            s[v, p + 1, :, pl.ds(base + LANE, TILE)] = section
            t_send[1, 0, slot, v, :, pl.ds(tbase, TILE)] = section[cells - 1 :, :]
            t_send[1, 1, slot, v, :, pl.ds(tbase, TILE)] = section[0:1, :]

    def second(p, slot, base, tbase):
        for v, stepped in enumerate(evaluate(s, 1, p, slot, base, tbase)):
            before = q[v, p + 1, :, pl.ds(base + LANE, TILE)]
            out[v, p, :, pl.ds(tbase, TILE)] = 0.5 * (before + stepped)

    def evaluate_chunk(work, index, which):
        h, c = index // per_half, index % per_half
        base = pl.multiple_of(h * wide + c * CHUNK, LANE)
        tbase = pl.multiple_of(index * CHUNK, LANE)
        for p in which:
            work(p, p, base, tbase)

    neighbours = has_up.astype(jnp.int32) + has_dn.astype(jnp.int32)

    @pl.when(jnp.logical_not(first_even))
    def _():
        pl.semaphore_wait(barrier, jnp.where(odd, neighbours, 0) + number_before([1, n_az - 1] + layer_peers))

    signal_axial(ready.at[1], odd)
    for d, slot in [(n_az - 1, 0), (1, 1)] + [(d, group_of(n_az - d)) for d in layer_peers]:

        @pl.when(jnp.logical_and(before(d), jnp.logical_not(direct(d))))
        def _(d=d, slot=slot):
            pl.semaphore_signal(ready.at[slot], inc=1, device_id={"az": sector_at(d)})

    parts = range(count)
    last = jnp.logical_or(az == 0, az == n_az - 1)
    others = [*range(edge), *range(edge + 2, count)]
    order = [*others[: edge - 1], edge, edge + 1, *others[edge - 1 :]]
    order_last = [*others, edge, edge + 1]

    def planes_start():
        for index, index_last in zip(order, order_last):
            axial_start(q, 0, jnp.where(last, index_last, index))

    @pl.when(odd)
    def _():
        @pl.when(has_up)
        def _():
            loaded(1, 1)

        @pl.when(has_dn)
        def _():
            loaded(1, 0)

        planes_start()

    loaded(planes - 2, 2)

    @pl.when(jnp.logical_or(even, jnp.logical_not(has_up)))
    def _():
        loaded(1, 1)

    @pl.when(jnp.logical_or(even, jnp.logical_not(has_dn)))
    def _():
        loaded(1, 0)


    def pack_rows(way):
        row = slice(0, 1) if way else slice(cells - 1, cells)
        for p in range(planes):
            for v in range(nv):
                for h in range(2):
                    lanes = slice(h * wide + LANE, h * wide + LANE + half)
                    t_send[0, way, p, v, :, h * half : (h + 1) * half] = q[v, p + 1, row, lanes]

    def sector_start(way):
        to_last = az <= 1 if way else az >= n_az - 2
        for index, index_last in zip(order, order_last):
            sector(0, way, jnp.where(to_last, index_last, index)).start()

    @pl.when(az == n_az - 1)
    def _():
        pack_rows(0)
        sector_start(0)

    pack_layers(q, 0)
    for d in layer_peers:

        @pl.when(before(d))
        def _(d=d):
            spread(0, d).start()

    @pl.when(az < n_az - 1)
    def _():
        pack_rows(0)

    pack_rows(1)

    @pl.when(az > 0)
    def _():
        sector_start(1)

    @pl.when(even)
    def _():
        pl.semaphore_wait(ready.at[1], neighbours)
        planes_start()

    @pl.when(jnp.logical_not(before(1)))
    def _():
        pl.semaphore_wait(ready.at[0], 1)
        sector_start(0)

    for field in (q, s):
        for v in range(nv):
            for p in range(planes):
                field[v, p + 1, :, 0:LANE] = zero
                field[v, p + 1, :, wide - LANE : wide + LANE] = jnp.zeros((cells, 2 * LANE), jnp.float32)
                field[v, p + 1, :, 2 * wide - LANE :] = zero

        @pl.when(jnp.logical_not(has_dn))
        def _(field=field):
            for v in range(nv):
                field[v, 0, :, :] = jnp.zeros((cells, 2 * wide), jnp.float32)

        @pl.when(jnp.logical_not(has_up))
        def _(field=field):
            for v in range(nv):
                field[v, planes + 1, :, :] = jnp.zeros((cells, 2 * wide), jnp.float32)

    early = jnp.where(2 * az < n_az - 2, count, 0)
    prepare(q, 0, early)

    @pl.when(first_even)
    def _():
        pl.semaphore_wait(barrier, 1 + len(layer_peers))

    for group in range(2, 2 + GROUPS):
        members = [d for d in layer_peers if group_of(d) == group]
        after = len(members) - number_before(members)

        @pl.when(jnp.logical_and(after > 0, jnp.logical_not(first_even)))
        def _(group=group, after=after):
            pl.semaphore_wait(ready.at[group], after)

        for d in members:

            @pl.when(jnp.logical_not(before(d)))
            def _(d=d):
                spread(0, d).start()

    @pl.when(first_odd)
    def _():
        pl.semaphore_wait(ready.at[1], 1)

    @pl.when(az == 0)
    def _():
        sector_start(1)

    prepare(q, early, count)

    def other(place):
        return place + jnp.where(place < edge, 0, 2)

    def first_chunk(index, send):
        planes_wait(halo_recv, index, 1)
        evaluate_chunk(first, index, range(planes))

        @pl.when(send)
        def _():
            axial_start(s, 1, index)

        for way in range(2):
            sector(1, way, index).start()

    def second_chunk(index):
        sector_wait(index)
        evaluate_chunk(second, index, range(1, planes - 1))
        planes_wait(ax_recv, index, 0)
        evaluate_chunk(second, index, (0, planes - 1))

    def run_first(low, high):
        @pl.loop(low, high)
        def _(place):
            first_chunk(other(place), jnp.logical_or(az != 1, place < edge - 1))

    def run_second(low, high):
        @pl.loop(low, high)
        def _(place):
            second_chunk(other(place))

            @pl.when(jnp.logical_and(az == 1, place == edge - 2))
            def _():
                for index in others[edge - 1 :]:
                    axial_start(s, 1, index)

    split = jnp.where(last, len(others), edge - 1)
    run_first(0, split)
    all_of(g_recv[0], ag_recv.at[0])
    unpack_ghosts(0)

    @pl.loop(edge, edge + 2)
    def _(index):
        first_chunk(index, True)

    pack_layers(s, 1)
    for d in layer_peers:
        spread(1, d).start()
    run_first(split, len(others))

    prepare(s)
    split = jnp.where(last, len(others), jnp.where(az == 1, edge, jnp.where(2 * az < n_az, edge + 1, edge - 1)))
    run_second(0, split)
    all_of(g_recv[1], ag_recv.at[1])
    unpack_ghosts(1)

    @pl.loop(edge, edge + 2)
    def _(index):
        second_chunk(index)

    run_second(split, len(others))

    for turn in range(2):
        all_of(g_recv[turn], ag_send.at[turn])

    @pl.when(jnp.logical_and(has_up, has_dn))
    def _():
        all_of(q.at[:, 0:6, :, 0:radial], halo_send.at[0])

    @pl.when(has_up != has_dn)
    def _():
        all_of(q.at[:, 0:4, :, 0:radial], halo_send.at[0])

    @pl.when(jnp.logical_not(jnp.logical_or(has_up, has_dn)))
    def _():
        all_of(q.at[:, 0:2, :, 0:radial], halo_send.at[0])


def shards(n_ax, n_az, state, rotor_offset, rotor_fraction):
    nv, planes, cells, radial = state.shape
    around = n_az * cells
    low, high = around // 4 + cells, 3 * around // 4 - cells - 1
    d_min, d_max = low // cells, high // cells + 1
    reach = d_max - d_min + 1
    wide = radial // 2 + 2 * LANE
    count = radial // CHUNK
    sem = pltpu.SemaphoreType.DMA
    return pl.pallas_call(
        functools.partial(kernel, n_ax, n_az, d_min, d_max),
        out_shape=jax.ShapeDtypeStruct(state.shape, state.dtype),
        in_specs=[
            pl.BlockSpec(memory_space=pltpu.SMEM),
            pl.BlockSpec(memory_space=pltpu.SMEM),
            pl.BlockSpec(memory_space=pltpu.HBM),
        ],
        out_specs=pl.BlockSpec(memory_space=pltpu.VMEM),
        scratch_shapes=[
            pltpu.VMEM((nv, planes + 2, cells, 2 * wide), jnp.float32),
            pltpu.VMEM((nv, planes + 2, cells, 2 * wide), jnp.float32),
            pltpu.VMEM(state.shape, jnp.float32),
            pltpu.VMEM(state.shape, jnp.float32),
            pltpu.VMEM(state.shape, jnp.float32),
            pltpu.VMEM((2, 2, planes, nv, 1, radial), jnp.float32),
            pltpu.VMEM((2, 2, planes, nv, 1, radial), jnp.float32),
            pltpu.VMEM((2, cells, LANE), jnp.float32),
            pltpu.VMEM((reach, cells, LANE), jnp.float32),
            pltpu.VMEM((reach, cells, LANE), jnp.float32),
            sem((3,)),
            sem((1,)),
            sem((2,)),
            sem((count,)),
            sem((count,)),
            sem((count,)),
            sem((2,)),
            pltpu.SemaphoreType.REGULAR((2 + GROUPS,)),
        ],
        compiler_params=pltpu.CompilerParams(collective_id=0, has_side_effects=True, vmem_limit_bytes=55_000_000),
    )(rotor_offset, rotor_fraction, state)


def solution(mesh):
    return jax.shard_map(
        functools.partial(shards, mesh.shape["ax"], mesh.shape["az"]),
        mesh=mesh,
        in_specs=(P(None, "ax", "az", None), P(), P()),
        out_specs=P(None, "ax", "az", None),
        check_vma=False,
    )
```

```python
import functools

import jax
import jax.numpy as jnp
from jax import lax
from jax.experimental import pallas as pl
from jax.experimental.pallas import tpu as pltpu
from jax.sharding import PartitionSpec as P

step_size = 0.2
base_viscosity = 0.05
eddy_coeff = 0.05

LANE = 128
TILE = 256
CHUNK = 256
GROUPS = 3


def kernel(n_ax, n_az, d_min, d_max, off_ref, frac_ref, state, out, q, s, pre_r, pre_t, pre_b, t_send, t_recv, g_send, g_recv0, g_recv1,
           load_sem, halo_send, ag_send, halo_recv, ag_recv, ready):
    nv, planes, cells, radial = state.shape
    assert 2 * planes == cells and planes >= 4
    half = radial // 2
    wide = half + 2 * LANE
    per_half = half // CHUNK
    count = 2 * per_half
    edge = per_half - 1
    g_recv = (g_recv0, g_recv1)
    ax = lax.axis_index("ax")
    az = lax.axis_index("az")
    has_up = ax < n_ax - 1
    has_dn = ax > 0
    nxt = lax.rem(az + 1, n_az)
    prv = lax.rem(az + n_az - 1, n_az)

    def load(first, number, h, slot):
        return pltpu.make_async_copy(
            state.at[:, pl.ds(first, number), :, pl.ds(h * half, half)],
            q.at[:, pl.ds(first + 1, number), :, pl.ds(h * wide + LANE, half)],
            load_sem.at[slot],
        )

    even = lax.rem(ax, 2) == 0
    odd = jnp.logical_not(even)
    bottom_loads = [load(0, 1, h, 0) for h in range(2)]
    top_loads = [load(planes - 1, 1, h, 1) for h in range(2)]

    @pl.when(even)
    def _():
        for copy in top_loads + bottom_loads:
            copy.start()

    @pl.when(odd)
    def _():
        for copy in bottom_loads + top_loads:
            copy.start()

    for h in range(2):
        load(1, planes - 2, h, 2).start()

    def all_of(ref, semaphore):
        pltpu.make_async_copy(ref, ref, semaphore).wait()

    def loaded(number, slot):
        all_of(out.at[:, pl.ds(0, number)], load_sem.at[slot])

    barrier = pltpu.get_barrier_semaphore()

    layer_peers = list(range(d_min, d_max + 1))
    first_even = jnp.logical_and(az == 0, even)
    first_odd = jnp.logical_and(az == 0, odd)

    def group_of(d):
        return 2 + (d - d_min) * GROUPS // len(layer_peers)

    def sector_at(d):
        return lax.rem(az + d, n_az)

    def before(d):
        return sector_at(d) < az

    def number_before(ds):
        return sum(before(d).astype(jnp.int32) for d in ds)

    def direct(d):
        return jnp.logical_and(jnp.logical_and(sector_at(d) == 0, even), d != n_az - 1)

    def signal_axial(semaphore, when):
        @pl.when(jnp.logical_and(when, has_up))
        def _():
            pl.semaphore_signal(semaphore, inc=1, device_id={"ax": ax + 1})

        @pl.when(jnp.logical_and(when, has_dn))
        def _():
            pl.semaphore_signal(semaphore, inc=1, device_id={"ax": ax - 1})

    signal_axial(barrier, even)
    for d in [1, n_az - 1] + layer_peers:

        @pl.when(jnp.logical_or(jnp.logical_not(before(d)), direct(d)))
        def _(d=d):
            pl.semaphore_signal(barrier, inc=1, device_id={"az": sector_at(d)})

    zero = jnp.zeros((cells, LANE), jnp.float32)

    sub = lax.broadcasted_iota(jnp.int32, (cells, TILE), 0)
    sub1 = lax.broadcasted_iota(jnp.int32, (cells, LANE), 0)
    lane1 = lax.broadcasted_iota(jnp.int32, (cells, LANE), 1)

    def axial(field, turn, index, up):
        h, c = index // per_half, index % per_half
        lanes = pl.ds(pl.multiple_of(h * wide + LANE + c * CHUNK, LANE), CHUNK)
        way = 0 if up else 1
        return pltpu.make_async_remote_copy(
            src_ref=field.at[:, planes if up else 1, :, lanes],
            dst_ref=field.at[:, 0 if up else planes + 1, :, lanes],
            send_sem=halo_send.at[0],
            recv_sem=halo_recv.at[turn, index],
            device_id={"ax": ax + 1 if up else ax - 1},
        )

    def axial_start(field, turn, index):
        @pl.when(has_up)
        def _():
            axial(field, turn, index, True).start()

        @pl.when(has_dn)
        def _():
            axial(field, turn, index, False).start()

    def halo_wait(turn, index):
        lanes = pl.ds(pl.multiple_of(index * CHUNK, LANE), CHUNK)

        @pl.when(jnp.logical_and(has_up, has_dn))
        def _():
            all_of(out.at[:, 0:3, :, lanes], halo_recv.at[turn, index])

        @pl.when(has_up != has_dn)
        def _():
            all_of(out.at[:, 0:2, :, lanes], halo_recv.at[turn, index])

        @pl.when(jnp.logical_not(jnp.logical_or(has_up, has_dn)))
        def _():
            all_of(out.at[:, 0:1, :, lanes], halo_recv.at[turn, index])

    def sector(turn, way, part):
        where = (slice(None), slice(None), slice(None), pl.ds(pl.multiple_of(part * CHUNK, LANE), CHUNK))
        return pltpu.make_async_remote_copy(
            src_ref=t_send.at[(turn, way) + where],
            dst_ref=t_recv.at[(turn, way) + where],
            send_sem=halo_send.at[0],
            recv_sem=halo_recv.at[turn, part],
            device_id={"az": nxt if way == 0 else prv},
        )

    def spread(turn, d):
        return pltpu.make_async_remote_copy(
            src_ref=g_send.at[turn],
            dst_ref=g_recv[turn].at[d - d_min],
            send_sem=ag_send.at[turn],
            recv_sem=ag_recv.at[turn],
            device_id={"az": lax.rem(az + d, n_az)},
        )

    def pack_layers(field, turn):
        packed = zero
        for v in range(nv):
            for p in range(planes):
                index = v * planes + p
                stator = field[v, p + 1, :, wide + LANE : wide + 2 * LANE]
                rotor = field[v, p + 1, :, wide - 2 * LANE : wide - LANE]
                other = nv * planes + index
                if index:
                    stator = pltpu.roll(stator, index, 1)
                packed = jnp.where(lane1 == index, stator, packed)
                packed = jnp.where(lane1 == other, pltpu.roll(rotor, other + 1, 1), packed)
        g_send[turn] = packed

    def unpack_ghosts(turn):
        off = off_ref[0]
        f = frac_ref[0]

        def window(a, b, shift):
            turned = lax.rem(2 * cells - shift, cells)
            return jnp.where(sub1 < cells - shift, pltpu.roll(a, turned, 0), pltpu.roll(b, turned, 0))

        def between(start, lo, hi):
            k = jnp.clip(lax.div(start, cells), d_min, d_max - 1)
            r = lax.rem(start, cells)
            a = g_recv[turn][n_az - k - d_min]
            b = g_recv[turn][n_az - k - 1 - d_min]
            return lo * window(a, b, r) + hi * window(a, b, r + 1)

        rot = between(off, 1.0 - f, f)
        sta = between(n_az * cells - off - 1, f, 1.0 - f)
        for v in range(nv):
            for p in range(planes):
                index = v * planes + p
                other = nv * planes + index
                ghost = jnp.where(lane1 == LANE - 1, pltpu.roll(rot, LANE - 1 - index, 1), 0.0)
                pre_r[v, p, :, half - LANE : half] += ghost
                pre_b[v, p, :, half - LANE : half] += ghost
                ghost = jnp.where(lane1 == 0, pltpu.roll(sta, LANE - other, 1), 0.0)
                pre_r[v, p, :, half : half + LANE] -= ghost
                pre_b[v, p, :, half : half + LANE] += ghost

    def prepare(field, low=0, high=count):
        @pl.loop(low, high)
        def _(index):
            h, c = index // per_half, index % per_half
            base = pl.multiple_of(h * wide + c * CHUNK, LANE)
            lanes = pl.ds(pl.multiple_of(index * CHUNK, LANE), TILE)
            for p in range(planes):
                for v in range(nv):
                    ext = field[v, p + 1, :, pl.ds(base, TILE + 2 * LANE)]
                    value = ext[:, LANE : LANE + TILE]
                    up_r = pltpu.roll(ext, TILE + 2 * LANE - 1, 1)[:, LANE : LANE + TILE]
                    dn_r = pltpu.roll(ext, 1, 1)[:, LANE : LANE + TILE]
                    up_t = jnp.where(sub == cells - 1, 0.0, pltpu.roll(value, cells - 1, 0))
                    dn_t = jnp.where(sub == 0, 0.0, pltpu.roll(value, 1, 0))
                    pre_r[v, p, :, lanes] = up_r - dn_r
                    pre_t[v, p, :, lanes] = up_t - dn_t
                    pre_b[v, p, :, lanes] = (up_t + dn_t) + (up_r + dn_r) - 6.0 * value

    def evaluate(field, turn, p, slot, base, tbase):
        rates = [0.5 * step_size * field[v, p + 1, :, pl.ds(base + LANE, TILE)] for v in range(3)]
        moved, seconds = [], []
        strain = None
        lanes = pl.ds(tbase, TILE)
        for v in range(nv):
            value = field[v, p + 1, :, pl.ds(base + LANE, TILE)]
            up_p = field[v, p + 2, :, pl.ds(base + LANE, TILE)]
            dn_p = field[v, p, :, pl.ds(base + LANE, TILE)]
            before = jnp.where(sub == 0, t_recv[turn, 0, slot, v, :, lanes], 0.0)
            after = jnp.where(sub == cells - 1, t_recv[turn, 1, slot, v, :, lanes], 0.0)
            across = (up_p - dn_p, pre_t[v, p, :, lanes] + (after - before), pre_r[v, p, :, lanes])
            seconds.append((up_p + dn_p) + (after + before) + pre_b[v, p, :, lanes])
            moved.append(value - (rates[0] * across[0] + rates[1] * across[1] + rates[2] * across[2]))
            if v < 3:
                square = across[0] * across[0] + across[1] * across[1] + across[2] * across[2]
                strain = square if strain is None else strain + square
        viscous = step_size * base_viscosity + (0.5 * step_size * eddy_coeff) * jnp.sqrt(strain)
        return [moved[v] + viscous * seconds[v] for v in range(nv)]

    def first(p, slot, base, tbase):
        for v, section in enumerate(evaluate(q, 0, p, slot, base, tbase)):
            s[v, p + 1, :, pl.ds(base + LANE, TILE)] = section
            t_send[1, 0, slot, v, :, pl.ds(tbase, TILE)] = section[cells - 1 :, :]
            t_send[1, 1, slot, v, :, pl.ds(tbase, TILE)] = section[0:1, :]

    def second(p, slot, base, tbase):
        for v, stepped in enumerate(evaluate(s, 1, p, slot, base, tbase)):
            before = q[v, p + 1, :, pl.ds(base + LANE, TILE)]
            out[v, p, :, pl.ds(tbase, TILE)] = 0.5 * (before + stepped)

    def evaluate_chunk(work, index):
        h, c = index // per_half, index % per_half
        base = pl.multiple_of(h * wide + c * CHUNK, LANE)
        tbase = pl.multiple_of(index * CHUNK, LANE)
        for p in range(planes):
            work(p, p, base, tbase)

    neighbours = has_up.astype(jnp.int32) + has_dn.astype(jnp.int32)

    @pl.when(jnp.logical_not(first_even))
    def _():
        pl.semaphore_wait(barrier, jnp.where(odd, neighbours, 0) + number_before([1, n_az - 1] + layer_peers))

    signal_axial(ready.at[1], odd)
    for d, slot in [(n_az - 1, 0), (1, 1)] + [(d, group_of(n_az - d)) for d in layer_peers]:

        @pl.when(jnp.logical_and(before(d), jnp.logical_not(direct(d))))
        def _(d=d, slot=slot):
            pl.semaphore_signal(ready.at[slot], inc=1, device_id={"az": sector_at(d)})

    parts = range(count)
    last = jnp.logical_or(az == 0, az == n_az - 1)
    others = [*range(edge), *range(edge + 2, count)]
    order = [*others[: edge - 1], edge, edge + 1, *others[edge - 1 :]]
    order_last = [*others, edge, edge + 1]

    def planes_start():
        for index, index_last in zip(order, order_last):
            axial_start(q, 0, jnp.where(last, index_last, index))

    @pl.when(odd)
    def _():
        @pl.when(has_up)
        def _():
            loaded(1, 1)

        @pl.when(has_dn)
        def _():
            loaded(1, 0)

        planes_start()

    loaded(planes - 2, 2)

    @pl.when(jnp.logical_or(even, jnp.logical_not(has_up)))
    def _():
        loaded(1, 1)

    @pl.when(jnp.logical_or(even, jnp.logical_not(has_dn)))
    def _():
        loaded(1, 0)


    def pack_rows(way):
        row = slice(0, 1) if way else slice(cells - 1, cells)
        for p in range(planes):
            for v in range(nv):
                for h in range(2):
                    lanes = slice(h * wide + LANE, h * wide + LANE + half)
                    t_send[0, way, p, v, :, h * half : (h + 1) * half] = q[v, p + 1, row, lanes]

    def sector_start(way):
        to_last = az <= 1 if way else az >= n_az - 2
        for index, index_last in zip(order, order_last):
            sector(0, way, jnp.where(to_last, index_last, index)).start()

    @pl.when(az == n_az - 1)
    def _():
        pack_rows(0)
        sector_start(0)

    pack_layers(q, 0)
    for d in layer_peers:

        @pl.when(before(d))
        def _(d=d):
            spread(0, d).start()

    @pl.when(az < n_az - 1)
    def _():
        pack_rows(0)

    pack_rows(1)

    @pl.when(az > 0)
    def _():
        sector_start(1)

    @pl.when(even)
    def _():
        pl.semaphore_wait(ready.at[1], neighbours)
        planes_start()

    @pl.when(jnp.logical_not(before(1)))
    def _():
        pl.semaphore_wait(ready.at[0], 1)
        sector_start(0)

    for field in (q, s):
        for v in range(nv):
            for p in range(planes):
                field[v, p + 1, :, 0:LANE] = zero
                field[v, p + 1, :, wide - LANE : wide + LANE] = jnp.zeros((cells, 2 * LANE), jnp.float32)
                field[v, p + 1, :, 2 * wide - LANE :] = zero

        @pl.when(jnp.logical_not(has_dn))
        def _(field=field):
            for v in range(nv):
                field[v, 0, :, :] = jnp.zeros((cells, 2 * wide), jnp.float32)

        @pl.when(jnp.logical_not(has_up))
        def _(field=field):
            for v in range(nv):
                field[v, planes + 1, :, :] = jnp.zeros((cells, 2 * wide), jnp.float32)

    early = jnp.where(2 * az < n_az - 2, count, 0)
    prepare(q, 0, early)

    @pl.when(first_even)
    def _():
        pl.semaphore_wait(barrier, 1 + len(layer_peers))

    for group in range(2, 2 + GROUPS):
        members = [d for d in layer_peers if group_of(d) == group]
        after = len(members) - number_before(members)

        @pl.when(jnp.logical_and(after > 0, jnp.logical_not(first_even)))
        def _(group=group, after=after):
            pl.semaphore_wait(ready.at[group], after)

        for d in members:

            @pl.when(jnp.logical_not(before(d)))
            def _(d=d):
                spread(0, d).start()

    @pl.when(first_odd)
    def _():
        pl.semaphore_wait(ready.at[1], 1)

    @pl.when(az == 0)
    def _():
        sector_start(1)

    prepare(q, early, count)

    def other(place):
        return place + jnp.where(place < edge, 0, 2)

    def first_chunk(index, send):
        halo_wait(0, index)
        evaluate_chunk(first, index)

        @pl.when(send)
        def _():
            axial_start(s, 1, index)

        for way in range(2):
            sector(1, way, index).start()

    def second_chunk(index):
        halo_wait(1, index)
        evaluate_chunk(second, index)

    def run_first(low, high):
        @pl.loop(low, high)
        def _(place):
            first_chunk(other(place), jnp.logical_or(az != 1, place < edge - 1))

    def run_second(low, high):
        @pl.loop(low, high)
        def _(place):
            second_chunk(other(place))

            @pl.when(jnp.logical_and(az == 1, place == edge - 2))
            def _():
                for index in others[edge - 1 :]:
                    axial_start(s, 1, index)

    split = jnp.where(last, len(others), edge - 1)
    run_first(0, split)
    all_of(g_recv[0], ag_recv.at[0])
    unpack_ghosts(0)

    @pl.loop(edge, edge + 2)
    def _(index):
        first_chunk(index, True)

    pack_layers(s, 1)
    for d in layer_peers:
        spread(1, d).start()
    run_first(split, len(others))

    prepare(s)
    split = jnp.where(last, len(others), jnp.where(az == 1, edge, jnp.where(2 * az < n_az, edge + 1, edge - 1)))
    run_second(0, split)
    all_of(g_recv[1], ag_recv.at[1])
    unpack_ghosts(1)

    @pl.loop(edge, edge + 2)
    def _(index):
        second_chunk(index)

    run_second(split, len(others))

    for turn in range(2):
        all_of(g_recv[turn], ag_send.at[turn])

    @pl.when(jnp.logical_and(has_up, has_dn))
    def _():
        all_of(q.at[:, 0:6, :, 0:radial], halo_send.at[0])

    @pl.when(has_up != has_dn)
    def _():
        all_of(q.at[:, 0:4, :, 0:radial], halo_send.at[0])

    @pl.when(jnp.logical_not(jnp.logical_or(has_up, has_dn)))
    def _():
        all_of(q.at[:, 0:2, :, 0:radial], halo_send.at[0])


def shards(n_ax, n_az, state, rotor_offset, rotor_fraction):
    nv, planes, cells, radial = state.shape
    around = n_az * cells
    low, high = around // 4 + cells, 3 * around // 4 - cells - 1
    d_min, d_max = low // cells, high // cells + 1
    reach = d_max - d_min + 1
    wide = radial // 2 + 2 * LANE
    count = radial // CHUNK
    sem = pltpu.SemaphoreType.DMA
    return pl.pallas_call(
        functools.partial(kernel, n_ax, n_az, d_min, d_max),
        out_shape=jax.ShapeDtypeStruct(state.shape, state.dtype),
        in_specs=[
            pl.BlockSpec(memory_space=pltpu.SMEM),
            pl.BlockSpec(memory_space=pltpu.SMEM),
            pl.BlockSpec(memory_space=pltpu.HBM),
        ],
        out_specs=pl.BlockSpec(memory_space=pltpu.VMEM),
        scratch_shapes=[
            pltpu.VMEM((nv, planes + 2, cells, 2 * wide), jnp.float32),
            pltpu.VMEM((nv, planes + 2, cells, 2 * wide), jnp.float32),
            pltpu.VMEM(state.shape, jnp.float32),
            pltpu.VMEM(state.shape, jnp.float32),
            pltpu.VMEM(state.shape, jnp.float32),
            pltpu.VMEM((2, 2, planes, nv, 1, radial), jnp.float32),
            pltpu.VMEM((2, 2, planes, nv, 1, radial), jnp.float32),
            pltpu.VMEM((2, cells, LANE), jnp.float32),
            pltpu.VMEM((reach, cells, LANE), jnp.float32),
            pltpu.VMEM((reach, cells, LANE), jnp.float32),
            sem((3,)),
            sem((1,)),
            sem((2,)),
            sem((2, count)),
            sem((2,)),
            pltpu.SemaphoreType.REGULAR((2 + GROUPS,)),
        ],
        compiler_params=pltpu.CompilerParams(collective_id=0, has_side_effects=True, vmem_limit_bytes=55_000_000),
    )(rotor_offset, rotor_fraction, state)


def solution(mesh):
    return jax.shard_map(
        functools.partial(shards, mesh.shape["ax"], mesh.shape["az"]),
        mesh=mesh,
        in_specs=(P(None, "ax", "az", None), P(), P()),
        out_specs=P(None, "ax", "az", None),
        check_vma=False,
    )
```

```python
import functools

import jax
import jax.numpy as jnp
from jax import lax
from jax.experimental import pallas as pl
from jax.experimental.pallas import tpu as pltpu
from jax.sharding import PartitionSpec as P

step_size = 0.2
base_viscosity = 0.05
eddy_coeff = 0.05

LANE = 128
TILE = 256
CHUNK = 256
GROUPS = 3


def kernel(n_ax, n_az, d_min, d_max, off_ref, frac_ref, state, out, q, s, pre_r, pre_t, pre_b, t_send, t_recv, g_send, g_recv0, g_recv1,
           load_sem, halo_send, ag_send, halo_recv, ag_recv, ready):
    nv, planes, cells, radial = state.shape
    assert 2 * planes == cells and planes >= 4
    half = radial // 2
    wide = half + 2 * LANE
    per_half = half // CHUNK
    count = 2 * per_half
    edge = per_half - 1
    g_recv = (g_recv0, g_recv1)
    ax = lax.axis_index("ax")
    az = lax.axis_index("az")
    has_up = ax < n_ax - 1
    has_dn = ax > 0
    nxt = lax.rem(az + 1, n_az)
    prv = lax.rem(az + n_az - 1, n_az)

    def load(first, number, h, slot):
        return pltpu.make_async_copy(
            state.at[:, pl.ds(first, number), :, pl.ds(h * half, half)],
            q.at[:, pl.ds(first + 1, number), :, pl.ds(h * wide + LANE, half)],
            load_sem.at[slot],
        )

    even = lax.rem(ax, 2) == 0
    odd = jnp.logical_not(even)
    bottom_loads = [load(0, 1, h, 0) for h in range(2)]
    top_loads = [load(planes - 1, 1, h, 1) for h in range(2)]

    @pl.when(even)
    def _():
        for copy in top_loads + bottom_loads:
            copy.start()

    @pl.when(odd)
    def _():
        for copy in bottom_loads + top_loads:
            copy.start()

    for h in range(2):
        load(1, planes - 2, h, 2).start()

    def all_of(ref, semaphore):
        pltpu.make_async_copy(ref, ref, semaphore).wait()

    def loaded(number, slot):
        all_of(out.at[:, pl.ds(0, number)], load_sem.at[slot])

    barrier = pltpu.get_barrier_semaphore()

    layer_peers = list(range(d_min, d_max + 1))
    first_even = jnp.logical_and(az == 0, even)
    first_odd = jnp.logical_and(az == 0, odd)

    def group_of(d):
        return 2 + (d - d_min) * GROUPS // len(layer_peers)

    def sector_at(d):
        return lax.rem(az + d, n_az)

    def before(d):
        return sector_at(d) < az

    def number_before(ds):
        return sum(before(d).astype(jnp.int32) for d in ds)

    def direct(d):
        return jnp.logical_and(jnp.logical_and(sector_at(d) == 0, even), d != n_az - 1)

    def signal_axial(semaphore, when):
        @pl.when(jnp.logical_and(when, has_up))
        def _():
            pl.semaphore_signal(semaphore, inc=1, device_id={"ax": ax + 1})

        @pl.when(jnp.logical_and(when, has_dn))
        def _():
            pl.semaphore_signal(semaphore, inc=1, device_id={"ax": ax - 1})

    signal_axial(barrier, even)
    for d in [1, n_az - 1] + layer_peers:

        @pl.when(jnp.logical_or(jnp.logical_not(before(d)), direct(d)))
        def _(d=d):
            pl.semaphore_signal(barrier, inc=1, device_id={"az": sector_at(d)})

    zero = jnp.zeros((cells, LANE), jnp.float32)

    sub = lax.broadcasted_iota(jnp.int32, (cells, TILE), 0)
    sub1 = lax.broadcasted_iota(jnp.int32, (cells, LANE), 0)
    lane1 = lax.broadcasted_iota(jnp.int32, (cells, LANE), 1)

    def axial(field, turn, index, up):
        h, c = index // per_half, index % per_half
        lanes = pl.ds(pl.multiple_of(h * wide + LANE + c * CHUNK, LANE), CHUNK)
        way = 0 if up else 1
        return pltpu.make_async_remote_copy(
            src_ref=field.at[:, planes if up else 1, :, lanes],
            dst_ref=field.at[:, 0 if up else planes + 1, :, lanes],
            send_sem=halo_send.at[0],
            recv_sem=halo_recv.at[turn, index],
            device_id={"ax": ax + 1 if up else ax - 1},
        )

    def axial_start(field, turn, index):
        @pl.when(has_up)
        def _():
            axial(field, turn, index, True).start()

        @pl.when(has_dn)
        def _():
            axial(field, turn, index, False).start()

    def halo_wait(turn, index):
        lanes = pl.ds(pl.multiple_of(index * CHUNK, LANE), CHUNK)

        @pl.when(jnp.logical_and(has_up, has_dn))
        def _():
            all_of(out.at[:, 0:3, :, lanes], halo_recv.at[turn, index])

        @pl.when(has_up != has_dn)
        def _():
            all_of(out.at[:, 0:2, :, lanes], halo_recv.at[turn, index])

        @pl.when(jnp.logical_not(jnp.logical_or(has_up, has_dn)))
        def _():
            all_of(out.at[:, 0:1, :, lanes], halo_recv.at[turn, index])

    def sector(turn, way, part):
        where = (slice(None), slice(None), slice(None), pl.ds(pl.multiple_of(part * CHUNK, LANE), CHUNK))
        return pltpu.make_async_remote_copy(
            src_ref=t_send.at[(turn, way) + where],
            dst_ref=t_recv.at[(turn, way) + where],
            send_sem=halo_send.at[0],
            recv_sem=halo_recv.at[turn, part],
            device_id={"az": nxt if way == 0 else prv},
        )

    def spread(turn, d):
        return pltpu.make_async_remote_copy(
            src_ref=g_send.at[turn],
            dst_ref=g_recv[turn].at[d - d_min],
            send_sem=ag_send.at[turn],
            recv_sem=ag_recv.at[turn],
            device_id={"az": lax.rem(az + d, n_az)},
        )

    def pack_layers(field, turn):
        packed = zero
        for v in range(nv):
            for p in range(planes):
                index = v * planes + p
                stator = field[v, p + 1, :, wide + LANE : wide + 2 * LANE]
                rotor = field[v, p + 1, :, wide - 2 * LANE : wide - LANE]
                other = nv * planes + index
                if index:
                    stator = pltpu.roll(stator, index, 1)
                packed = jnp.where(lane1 == index, stator, packed)
                packed = jnp.where(lane1 == other, pltpu.roll(rotor, other + 1, 1), packed)
        g_send[turn] = packed

    def unpack_ghosts(turn):
        off = off_ref[0]
        f = frac_ref[0]

        def window(a, b, shift):
            turned = lax.rem(2 * cells - shift, cells)
            return jnp.where(sub1 < cells - shift, pltpu.roll(a, turned, 0), pltpu.roll(b, turned, 0))

        def between(start, lo, hi):
            k = jnp.clip(lax.div(start, cells), d_min, d_max - 1)
            r = lax.rem(start, cells)
            a = g_recv[turn][n_az - k - d_min]
            b = g_recv[turn][n_az - k - 1 - d_min]
            return lo * window(a, b, r) + hi * window(a, b, r + 1)

        rot = between(off, 1.0 - f, f)
        sta = between(n_az * cells - off - 1, f, 1.0 - f)
        for v in range(nv):
            for p in range(planes):
                index = v * planes + p
                other = nv * planes + index
                ghost = jnp.where(lane1 == LANE - 1, pltpu.roll(rot, LANE - 1 - index, 1), 0.0)
                pre_r[v, p, :, half - LANE : half] += ghost
                pre_b[v, p, :, half - LANE : half] += ghost
                ghost = jnp.where(lane1 == 0, pltpu.roll(sta, LANE - other, 1), 0.0)
                pre_r[v, p, :, half : half + LANE] -= ghost
                pre_b[v, p, :, half : half + LANE] += ghost

    def prepare(field, low=0, high=count):
        @pl.loop(low, high)
        def _(index):
            h, c = index // per_half, index % per_half
            base = pl.multiple_of(h * wide + c * CHUNK, LANE)
            lanes = pl.ds(pl.multiple_of(index * CHUNK, LANE), TILE)
            for p in range(planes):
                for v in range(nv):
                    ext = field[v, p + 1, :, pl.ds(base, TILE + 2 * LANE)]
                    value = ext[:, LANE : LANE + TILE]
                    up_r = pltpu.roll(ext, TILE + 2 * LANE - 1, 1)[:, LANE : LANE + TILE]
                    dn_r = pltpu.roll(ext, 1, 1)[:, LANE : LANE + TILE]
                    up_t = jnp.where(sub == cells - 1, 0.0, pltpu.roll(value, cells - 1, 0))
                    dn_t = jnp.where(sub == 0, 0.0, pltpu.roll(value, 1, 0))
                    pre_r[v, p, :, lanes] = up_r - dn_r
                    pre_t[v, p, :, lanes] = up_t - dn_t
                    pre_b[v, p, :, lanes] = (up_t + dn_t) + (up_r + dn_r) - 6.0 * value

    def evaluate(field, turn, p, slot, base, tbase):
        rates = [0.5 * step_size * field[v, p + 1, :, pl.ds(base + LANE, TILE)] for v in range(3)]
        moved, seconds = [], []
        strain = None
        lanes = pl.ds(tbase, TILE)
        for v in range(nv):
            value = field[v, p + 1, :, pl.ds(base + LANE, TILE)]
            up_p = field[v, p + 2, :, pl.ds(base + LANE, TILE)]
            dn_p = field[v, p, :, pl.ds(base + LANE, TILE)]
            before = jnp.where(sub == 0, t_recv[turn, 0, slot, v, :, lanes], 0.0)
            after = jnp.where(sub == cells - 1, t_recv[turn, 1, slot, v, :, lanes], 0.0)
            across = (up_p - dn_p, pre_t[v, p, :, lanes] + (after - before), pre_r[v, p, :, lanes])
            seconds.append((up_p + dn_p) + (after + before) + pre_b[v, p, :, lanes])
            moved.append(value - (rates[0] * across[0] + rates[1] * across[1] + rates[2] * across[2]))
            if v < 3:
                square = across[0] * across[0] + across[1] * across[1] + across[2] * across[2]
                strain = square if strain is None else strain + square
        viscous = step_size * base_viscosity + (0.5 * step_size * eddy_coeff) * jnp.sqrt(strain)
        return [moved[v] + viscous * seconds[v] for v in range(nv)]

    def first(p, slot, base, tbase):
        for v, section in enumerate(evaluate(q, 0, p, slot, base, tbase)):
            s[v, p + 1, :, pl.ds(base + LANE, TILE)] = section
            t_send[1, 0, slot, v, :, pl.ds(tbase, TILE)] = section[cells - 1 :, :]
            t_send[1, 1, slot, v, :, pl.ds(tbase, TILE)] = section[0:1, :]

    def second(p, slot, base, tbase):
        for v, stepped in enumerate(evaluate(s, 1, p, slot, base, tbase)):
            before = q[v, p + 1, :, pl.ds(base + LANE, TILE)]
            out[v, p, :, pl.ds(tbase, TILE)] = 0.5 * (before + stepped)

    def evaluate_chunk(work, index):
        h, c = index // per_half, index % per_half
        base = pl.multiple_of(h * wide + c * CHUNK, LANE)
        tbase = pl.multiple_of(index * CHUNK, LANE)
        for p in range(planes):
            work(p, p, base, tbase)

    neighbours = has_up.astype(jnp.int32) + has_dn.astype(jnp.int32)

    @pl.when(jnp.logical_not(first_even))
    def _():
        pl.semaphore_wait(barrier, jnp.where(odd, neighbours, 0) + number_before([1, n_az - 1] + layer_peers))

    signal_axial(ready.at[1], odd)
    for d, slot in [(n_az - 1, 0), (1, 1)] + [(d, group_of(n_az - d)) for d in layer_peers]:

        @pl.when(jnp.logical_and(before(d), jnp.logical_not(direct(d))))
        def _(d=d, slot=slot):
            pl.semaphore_signal(ready.at[slot], inc=1, device_id={"az": sector_at(d)})

    parts = range(count)
    last = jnp.logical_or(az == 0, az == n_az - 1)
    others = [*range(edge), *range(edge + 2, count)]
    order = [*others[: edge - 1], edge, edge + 1, *others[edge - 1 :]]
    order_last = [*others, edge, edge + 1]

    def planes_start():
        for index, index_last in zip(order, order_last):
            axial_start(q, 0, jnp.where(last, index_last, index))

    @pl.when(odd)
    def _():
        @pl.when(has_up)
        def _():
            loaded(1, 1)

        @pl.when(has_dn)
        def _():
            loaded(1, 0)

        planes_start()

    loaded(planes - 2, 2)

    @pl.when(jnp.logical_or(even, jnp.logical_not(has_up)))
    def _():
        loaded(1, 1)

    @pl.when(jnp.logical_or(even, jnp.logical_not(has_dn)))
    def _():
        loaded(1, 0)


    def pack_rows(way):
        row = slice(0, 1) if way else slice(cells - 1, cells)
        for p in range(planes):
            for v in range(nv):
                for h in range(2):
                    lanes = slice(h * wide + LANE, h * wide + LANE + half)
                    t_send[0, way, p, v, :, h * half : (h + 1) * half] = q[v, p + 1, row, lanes]

    def sector_start(way):
        to_last = az <= 1 if way else az >= n_az - 2
        for index, index_last in zip(order, order_last):
            sector(0, way, jnp.where(to_last, index_last, index)).start()

    @pl.when(az == n_az - 1)
    def _():
        pack_rows(0)
        sector_start(0)

    pack_layers(q, 0)
    for d in layer_peers:

        @pl.when(before(d))
        def _(d=d):
            spread(0, d).start()

    @pl.when(az < n_az - 1)
    def _():
        pack_rows(0)

    pack_rows(1)

    @pl.when(az > 0)
    def _():
        sector_start(1)

    @pl.when(even)
    def _():
        pl.semaphore_wait(ready.at[1], neighbours)
        planes_start()

    @pl.when(jnp.logical_not(before(1)))
    def _():
        pl.semaphore_wait(ready.at[0], 1)
        sector_start(0)

    for field in (q, s):
        for v in range(nv):
            for p in range(planes):
                field[v, p + 1, :, 0:LANE] = zero
                field[v, p + 1, :, wide - LANE : wide + LANE] = jnp.zeros((cells, 2 * LANE), jnp.float32)
                field[v, p + 1, :, 2 * wide - LANE :] = zero

        @pl.when(jnp.logical_not(has_dn))
        def _(field=field):
            for v in range(nv):
                field[v, 0, :, :] = jnp.zeros((cells, 2 * wide), jnp.float32)

        @pl.when(jnp.logical_not(has_up))
        def _(field=field):
            for v in range(nv):
                field[v, planes + 1, :, :] = jnp.zeros((cells, 2 * wide), jnp.float32)

    early = jnp.where(2 * az < n_az - 2, count, 0)
    prepare(q, 0, early)

    @pl.when(first_even)
    def _():
        pl.semaphore_wait(barrier, 1 + len(layer_peers))

    for group in range(2, 2 + GROUPS):
        members = [d for d in layer_peers if group_of(d) == group]
        after = len(members) - number_before(members)

        @pl.when(jnp.logical_and(after > 0, jnp.logical_not(first_even)))
        def _(group=group, after=after):
            pl.semaphore_wait(ready.at[group], after)

        for d in members:

            @pl.when(jnp.logical_not(before(d)))
            def _(d=d):
                spread(0, d).start()

    @pl.when(first_odd)
    def _():
        pl.semaphore_wait(ready.at[1], 1)

    @pl.when(az == 0)
    def _():
        sector_start(1)

    prepare(q, early, count)

    def other(place):
        return place + jnp.where(place < edge, 0, 2)

    def first_chunk(index, send):
        halo_wait(0, index)
        evaluate_chunk(first, index)

        @pl.when(send)
        def _():
            axial_start(s, 1, index)

        for way in range(2):
            sector(1, way, index).start()

    def second_chunk(index):
        halo_wait(1, index)
        evaluate_chunk(second, index)

    def run_first(low, high):
        @pl.loop(low, high)
        def _(place):
            first_chunk(other(place), jnp.logical_or(az != 1, place < edge - 1))

    def run_second(low, high):
        @pl.loop(low, high)
        def _(place):
            @pl.when(jnp.logical_and(az == 1, place == edge - 2))
            def _():
                for index in others[edge - 1 :]:
                    axial_start(s, 1, index)

            second_chunk(other(place))

    split = jnp.where(last, len(others), edge - 1)
    run_first(0, split)
    all_of(g_recv[0], ag_recv.at[0])
    unpack_ghosts(0)

    @pl.loop(edge, edge + 2)
    def _(index):
        first_chunk(index, True)

    pack_layers(s, 1)
    for d in layer_peers:
        spread(1, d).start()
    run_first(split, len(others))

    prepare(s)
    split = jnp.where(last, len(others), jnp.where(az == 1, edge, jnp.where(2 * az < n_az, edge + 1, edge - 1)))
    run_second(0, split)
    all_of(g_recv[1], ag_recv.at[1])
    unpack_ghosts(1)

    @pl.loop(edge, edge + 2)
    def _(index):
        second_chunk(index)

    run_second(split, len(others))

    for turn in range(2):
        all_of(g_recv[turn], ag_send.at[turn])

    @pl.when(jnp.logical_and(has_up, has_dn))
    def _():
        all_of(q.at[:, 0:6, :, 0:radial], halo_send.at[0])

    @pl.when(has_up != has_dn)
    def _():
        all_of(q.at[:, 0:4, :, 0:radial], halo_send.at[0])

    @pl.when(jnp.logical_not(jnp.logical_or(has_up, has_dn)))
    def _():
        all_of(q.at[:, 0:2, :, 0:radial], halo_send.at[0])


def shards(n_ax, n_az, state, rotor_offset, rotor_fraction):
    nv, planes, cells, radial = state.shape
    around = n_az * cells
    low, high = around // 4 + cells, 3 * around // 4 - cells - 1
    d_min, d_max = low // cells, high // cells + 1
    reach = d_max - d_min + 1
    wide = radial // 2 + 2 * LANE
    count = radial // CHUNK
    sem = pltpu.SemaphoreType.DMA
    return pl.pallas_call(
        functools.partial(kernel, n_ax, n_az, d_min, d_max),
        out_shape=jax.ShapeDtypeStruct(state.shape, state.dtype),
        in_specs=[
            pl.BlockSpec(memory_space=pltpu.SMEM),
            pl.BlockSpec(memory_space=pltpu.SMEM),
            pl.BlockSpec(memory_space=pltpu.HBM),
        ],
        out_specs=pl.BlockSpec(memory_space=pltpu.VMEM),
        scratch_shapes=[
            pltpu.VMEM((nv, planes + 2, cells, 2 * wide), jnp.float32),
            pltpu.VMEM((nv, planes + 2, cells, 2 * wide), jnp.float32),
            pltpu.VMEM(state.shape, jnp.float32),
            pltpu.VMEM(state.shape, jnp.float32),
            pltpu.VMEM(state.shape, jnp.float32),
            pltpu.VMEM((2, 2, planes, nv, 1, radial), jnp.float32),
            pltpu.VMEM((2, 2, planes, nv, 1, radial), jnp.float32),
            pltpu.VMEM((2, cells, LANE), jnp.float32),
            pltpu.VMEM((reach, cells, LANE), jnp.float32),
            pltpu.VMEM((reach, cells, LANE), jnp.float32),
            sem((3,)),
            sem((1,)),
            sem((2,)),
            sem((2, count)),
            sem((2,)),
            pltpu.SemaphoreType.REGULAR((2 + GROUPS,)),
        ],
        compiler_params=pltpu.CompilerParams(collective_id=0, has_side_effects=True, vmem_limit_bytes=55_000_000),
    )(rotor_offset, rotor_fraction, state)


def solution(mesh):
    return jax.shard_map(
        functools.partial(shards, mesh.shape["ax"], mesh.shape["az"]),
        mesh=mesh,
        in_specs=(P(None, "ax", "az", None), P(), P()),
        out_specs=P(None, "ax", "az", None),
        check_vma=False,
    )
```
